256 devices in a mesh: group: 32 (over z, y_hi, core), mp: 8 (over x, y_lo).
Axes of the slice: x: 4, y: 4 (y_hi: 2, y_lo: 2; y = y_hi * 2 + y_lo), z: 8, core: 2. Of those that a mesh axis runs over, the one named last changes fastest.
Arguments:
- anchor: float32 [16, 2048, 2048], P(None, 'group', 'mp'), may hold values from -6 to 6
- momentum: float32 [16, 2048, 2048], P(None, 'group', 'mp'), may hold values from -3 to 3
- deltas: float32 [32, 2, 2048, 2048], P('group', None, None, 'mp'), may hold values from -3 to 3
- old_path: int32 [32, 2], replicated, may hold values from 0 to 7, as said below
- new_path: int32 [32, 2], replicated, may hold values from 0 to 7, as said below
- tokens: bfloat16 [32, 1024, 2048], P('group', None, 'mp'), may hold values from -40 to 40
- cotangent: bfloat16 [32, 1024, 2048], P('group', None, 'mp'), may hold values from -6 to 6
Outputs:
- new_anchor: float32 [16, 2048, 2048], P(None, 'group', 'mp')
- new_momentum: float32 [16, 2048, 2048], P(None, 'group', 'mp')
- grads: bfloat16 [32, 2, 2048, 2048], P('group', None, None, 'mp')
The draws below stay inside these ranges and needn't reach their ends.
Inputs may be any that keep to these rules, and one draw needn't show every extreme that they name: `old_path`: for each of the 2 levels, every one of the 8 modules is named by at least one group. `new_path`: for each of the 2 levels, every one of the 8 modules is named by at least one group.
All inputs are finite; a program needn't handle non-finite values.
Results may differ from the reference program's by a relative error of at most 0.014.
Values may be sent and summed in bfloat16 or wider, within the bound.
A program may use at most 128 MiB of HBM per device.

```python
import math
import jax
import jax.numpy as jnp
from jax import lax

D = 2048
MODS = 8
LEVELS = 2
ROWS = 1024
GROUPS = 32
MODULES = 16
N_MP = 8


def path_table(key):
    columns = []
    for level in range(LEVELS):
        level_key = jax.random.fold_in(key, level)
        first_key, second_key, third_key, label_key, order_key = jax.random.split(level_key, 5)
        first = jax.random.randint(first_key, (GROUPS,), 0, MODS)
        second = jax.random.randint(second_key, (GROUPS,), 0, MODS)
        third = jax.random.randint(third_key, (GROUPS,), 0, MODS)
        skewed = jnp.minimum(jnp.minimum(first, second), third)
        positions = jnp.arange(GROUPS, dtype=jnp.int32)
        base = jnp.where(positions < MODS, positions, skewed)
        labels = jax.random.permutation(label_key, MODS)
        order = jax.random.permutation(order_key, GROUPS)
        columns.append(labels[base][order])
    return jnp.stack(columns, axis=1).astype(jnp.int32)


def draw_old_path(key, part):
    return path_table(jax.random.fold_in(key, 11))


def draw_new_path(key, part):
    return path_table(jax.random.fold_in(key, 23))


def draw_tokens(key, part):
    base_key, rough_key = jax.random.split(jax.random.fold_in(key, 37), 2)
    rough = jax.random.uniform(rough_key, (D,), jnp.float32, 0.7, 1.4)
    ramp = jnp.exp(jnp.linspace(math.log(0.2), math.log(2.0), D)).astype(jnp.float32)
    base = jnp.clip(jax.random.normal(base_key, (GROUPS, ROWS, D), jnp.float32), -4.5, 4.5)
    values = base * ramp * rough
    return values.astype(jnp.bfloat16)


def with_spikes(entries, stream_key, source, target, blocks, factor):
    owner, partner = [(jnp.arange(entries.shape[axis_at]) // (entries.shape[axis_at] // blocks)).reshape([-1 if axis == axis_at else 1 for axis in range(entries.ndim)]) for axis_at in (source, target)]
    chosen = jax.random.permutation(stream_key, blocks)[partner]
    strong = (owner == chosen) | (owner == (partner + blocks // 2) % blocks)
    return jnp.where(strong, factor * entries, entries)


def steps_of(rng, shape, cuts, smallest, top_value):
    def one(position, parts):
        draws = jax.random.uniform(jax.random.fold_in(jax.random.fold_in(rng, 6), position), (parts,), jnp.float32, smallest / len(cuts), top_value / len(cuts))
        return jnp.repeat(jnp.exp(draws), shape[position] // parts).reshape((-1,) + (1,) * (len(shape) - position - 1))

    loudness = one(*cuts[0])
    for cut in cuts[1:]:
        loudness = loudness * one(*cut)
    return loudness


def noise(stream_key, shape, width, most, pieces=(), kind=jnp.bfloat16):
    array = jax.random.normal(stream_key, shape, jnp.float32) * width
    if len(pieces) > 0:
        array = steps_of(stream_key, shape, pieces, -0.22, 0.18) * array
    return jnp.clip(array, min=-most, max=most).astype(kind)


def heavy_noise(key, shape, spread, reach, shards, heavy, held_as=jnp.bfloat16):
    values = spread * jax.random.normal(key, shape, jnp.float32)
    if shards:
        values = values * steps_of(key, shape, shards, -0.22, 0.18)
    return jnp.clip(with_spikes(values, jax.random.fold_in(key, 3), *heavy), -reach, reach).astype(held_as)


def setup_inputs(seed: int = 0) -> dict:
    seeds = jax.random.split(jax.random.key(seed), 8)
    anchor = noise(seeds[0], (MODULES, D, D), 1.0, 6.0, ((1, 32), (2, 8)), jnp.float32)
    momentum = noise(seeds[1], (MODULES, D, D), 0.5, 3.0, ((1, 32), (2, 8)), jnp.float32)
    deltas = heavy_noise(seeds[2], (GROUPS, LEVELS, D, D), 0.5, 3.0, ((0, 32), (3, 8)), (0, 2, 32, 2.75), jnp.float32)
    old_path = draw_old_path(jax.random.fold_in(seeds[7], 71), 0)
    new_path = draw_new_path(jax.random.fold_in(seeds[7], 71), 0)
    tokens = draw_tokens(jax.random.fold_in(seeds[7], 71), 0)
    cotangent = noise(seeds[6], (GROUPS, ROWS, D), 1.0, 6.0, ((0, 32), (2, 8)))
    return {"anchor": anchor, "momentum": momentum, "deltas": deltas, "old_path": old_path, "new_path": new_path, "tokens": tokens, "cotangent": cotangent}


outer_rate = 0.7
momentum_rate = 0.9
epsilon = 1e-06

def silu_slope(values):
    sigmoid_part = jax.nn.sigmoid(values)
    return sigmoid_part * (1.0 + values * (1.0 - sigmoid_part))

def normalize(hidden):
    mean_square = lax.optimization_barrier(jnp.mean(hidden * hidden, axis=-1))
    scale = lax.rsqrt(mean_square + epsilon)
    return ((hidden * scale[:, None]).astype(jnp.bfloat16), scale)

def reference(anchor, momentum, deltas, old_path, new_path, tokens, cotangent):
    factor = 1.0 / math.sqrt(D)
    level_offsets = jnp.arange(LEVELS, dtype=jnp.int32) * MODS
    old_index = (old_path + level_offsets[None, :]).astype(jnp.int32).reshape(-1)
    flat_deltas = deltas.reshape(GROUPS * LEVELS, D, D)
    sums = jax.ops.segment_sum(flat_deltas, old_index, num_segments=MODULES)
    counts = jax.ops.segment_sum(jnp.ones((GROUPS * LEVELS,), jnp.float32), old_index, num_segments=MODULES)
    outer_grad = sums / counts[:, None, None]
    new_momentum = momentum_rate * momentum + outer_grad
    new_anchor = anchor - outer_rate * (outer_grad + momentum_rate * new_momentum)
    new_index = (new_path + level_offsets[None, :]).astype(jnp.int32)

    def one_group(inputs):
        tokens_row, grad_row, index_row = inputs
        first_weight = lax.dynamic_index_in_dim(new_anchor, index_row[0], 0, keepdims=False).astype(jnp.bfloat16)
        second_weight = lax.dynamic_index_in_dim(new_anchor, index_row[1], 0, keepdims=False).astype(jnp.bfloat16)
        first_state = tokens_row.astype(jnp.float32)
        first_normed, first_scale = normalize(first_state)
        first_pre = jnp.dot(first_normed, first_weight, preferred_element_type=jnp.float32) * factor
        second_state = (first_state + jax.nn.silu(first_pre)).astype(jnp.bfloat16).astype(jnp.float32)
        second_normed, second_scale = normalize(second_state)
        second_pre = jnp.dot(second_normed, second_weight, preferred_element_type=jnp.float32) * factor
        upstream = grad_row.astype(jnp.float32)
        second_slope = (upstream * silu_slope(second_pre)).astype(jnp.bfloat16)
        second_grad = (lax.dot_general(second_normed, second_slope, (((0,), (0,)), ((), ())), preferred_element_type=jnp.float32) * factor).astype(jnp.bfloat16)
        slope_blocks = second_slope.astype(jnp.float32).reshape(ROWS, N_MP, D // N_MP)
        weight_blocks = second_weight.astype(jnp.float32).reshape(D, N_MP, D // N_MP)
        partial_terms = jnp.einsum('rpc,dpc->prd', slope_blocks, weight_blocks, precision=lax.Precision.HIGHEST) * factor
        rounded = lax.optimization_barrier(partial_terms.astype(jnp.bfloat16)).astype(jnp.float32)
        normed_grad = lax.optimization_barrier(jnp.sum(rounded, axis=0))
        inner = lax.optimization_barrier(jnp.sum(normed_grad * second_state, axis=-1))
        state_grad = upstream + second_scale[:, None] * normed_grad - second_state * (second_scale ** 3 * inner / D)[:, None]
        first_slope = (state_grad * silu_slope(first_pre)).astype(jnp.bfloat16)
        first_grad = (lax.dot_general(first_normed, first_slope, (((0,), (0,)), ((), ())), preferred_element_type=jnp.float32) * factor).astype(jnp.bfloat16)
        return jnp.stack([first_grad, second_grad])
    grads = lax.map(one_group, (tokens, cotangent, new_index))
    return (new_anchor, new_momentum, grads)
```

```python
import math

import jax
import jax.numpy as jnp
from jax import lax
from jax.experimental import pallas as pl
from jax.experimental.pallas import tpu as pltpu
from jax.sharding import Mesh
from jax.sharding import PartitionSpec as P

D = 2048
MODS = 8
GROUPS = 32
ROWS = 1024
LEVELS = 2
BLOCK = D // GROUPS
WIDTH = 256
PARTS = D // WIDTH
CHUNKS = 4
CHUNK = ROWS // CHUNKS
HALF = CHUNK // 2
TILE = 16
FACTOR = 1.0 / math.sqrt(D)

outer_rate = 0.7
momentum_rate = 0.9
epsilon = 1e-06

AXES = ("z", "yh", "c", "x", "yl")
SIZES = (8, 2, 2, 4, 2)
GROUP = ("z", "yh", "c")
MP = ("x", "yl")
NEAR = (3, -3, 2, -2, 1, -1, 0)
RELAYS = 18
BF16 = jnp.bfloat16
F32 = jnp.float32


def wrap(value, size):
    return lax.rem(value + size, size)


def sigmoid(values):
    return 1.0 / (1.0 + jnp.exp(-values))


def silu_slope(values):
    part = sigmoid(values)
    return part * (1.0 + values * (1.0 - part))


def dot(a, b, dims):
    return lax.dot_general(a, b, ((dims[0:1], dims[1:2]), ((), ())), preferred_element_type=F32)


def kernel(
    old_ref,
    new_ref,
    anchor_ref,
    momentum_ref,
    deltas_ref,
    tokens_ref,
    cot_ref,
    out_anchor,
    out_momentum,
    out_grads,
    raw,
    send,
    recv,
    relay,
    anchor,
    momentum,
    modules,
    tok,
    cot,
    state,
    pre0,
    scale0,
    scale1,
    slopes,
    terms,
    ra,
    rb,
    rc,
    inner,
    acc,
    gout,
    load_sem,
    store_sem,
    send_sem,
    relay_sem,
    recv_sem,
    tok_sem,
    state_sem,
    rs_sem,
    inner_sem,
):
    z = lax.axis_index("z")
    yh = lax.axis_index("yh")
    c = lax.axis_index("c")
    x = lax.axis_index("x")
    yl = lax.axis_index("yl")
    y = yh * 2 + yl
    group = z * 4 + yh * 2 + c
    mine = x * 2 + yl

    def remote(src, dst, sender, receiver, device):
        return pltpu.make_async_remote_copy(
            src_ref=src,
            dst_ref=dst,
            send_sem=sender,
            recv_sem=receiver,
            device_id=device,
            device_id_type=pl.DeviceIdType.MESH,
        )

    def wait_bytes(ref, sem):
        pltpu.make_async_copy(ref, ref, sem).wait()

    def place(dz, dy, core):
        there = wrap(y + dy, 4)
        return (wrap(z + dz, 8), there // 2, core, x, lax.rem(there, 2))

    def send_blocks(p):
        def go(dz, cross, core, dst, receiver, device):
            target = wrap(z + dz, 8) * 4 + lax.rem(yh + cross, 2) * 2 + core
            remote(send.at[p, target], dst, send_sem.at[p], receiver, device).start()

        for i, sign in enumerate((1, -1)):
            go(4, 1, i, relay.at[p, 14 + i], relay_sem.at[p, 14 + i], place(2 * sign, sign, c))
            go(4, 0, i, relay.at[p, 16 + i], relay_sem.at[p, 16 + i], place(2 * sign, 0, c))
        for j, dz in enumerate(NEAR):
            for i, sign in enumerate((1, -1)):
                slot = i * 7 + j
                go(dz, 1, i, relay.at[p, slot], relay_sem.at[p, slot], place(dz, sign, c))
        for dz in NEAR:
            if dz == 0:
                go(0, 0, 1 - c, recv.at[p, group], recv_sem.at[p], place(0, 0, 1 - c))
            else:
                for i in range(2):
                    go(dz, 0, i, recv.at[p, group], recv_sem.at[p], place(dz, 0, i))

    def forward_blocks(p):
        def go(slot, dz, dy, device):
            source = wrap(z - dz, 8) * 4 + (wrap(y - dy, 4) // 2) * 2 + c
            wait_bytes(relay.at[p, slot], relay_sem.at[p, slot])
            remote(
                relay.at[p, slot], recv.at[p, source], send_sem.at[4 + p], recv_sem.at[p], device
            ).start()

        for i, sign in enumerate((1, -1)):
            go(14 + i, 2 * sign, sign, place(2 * sign, sign, i))
            go(16 + i, 2 * sign, 0, place(2 * sign, 0, i))
        for j, dz in enumerate(NEAR):
            for i, sign in enumerate((1, -1)):
                go(i * 7 + j, dz, sign, place(0, sign, i))

    def update(l):
        wait_bytes(recv.at[l, pl.ds(0, GROUPS - 1)], recv_sem.at[l])

        def count_one(g, counts):
            named = old_ref[g, l]
            return tuple(n + jnp.where(named == m, 1.0, 0.0) for m, n in enumerate(counts))

        counts = lax.fori_loop(0, GROUPS, count_one, (jnp.float32(0.0),) * MODS)

        def rows_of(r, carry):
            rows = pl.ds(pl.multiple_of(r * TILE, TILE), TILE)

            def add_one(g, sums):
                named = old_ref[g, l]
                value = recv[l, g, rows, :].astype(F32)
                return tuple(
                    s + value * jnp.where(named == m, 1.0, 0.0) for m, s in enumerate(sums)
                )

            sums = lax.fori_loop(
                0, GROUPS, add_one, (jnp.zeros((TILE, WIDTH), F32),) * MODS
            )
            for m in range(MODS):
                k = l * MODS + m
                outer_grad = sums[m] / counts[m]
                fresh = momentum_rate * momentum[k, rows, :] + outer_grad
                moved = anchor[k, rows, :] - outer_rate * (outer_grad + momentum_rate * fresh)
                momentum[k, rows, :] = fresh
                anchor[k, rows, :] = moved
                modules[k, rows, :] = moved.astype(BF16)
            return carry

        lax.fori_loop(0, BLOCK // TILE, rows_of, 0)

        def stage(g, carry):
            send[2 + l, g] = modules[l * MODS + new_ref[g, l]]
            return carry

        lax.fori_loop(0, GROUPS, stage, 0)
        recv[2 + l, group] = modules[l * MODS + new_ref[group, l]]
        part = pl.ds(l * MODS, MODS)
        pltpu.make_async_copy(anchor.at[part], out_anchor.at[part], store_sem.at[l]).start()
        pltpu.make_async_copy(momentum.at[part], out_momentum.at[part], store_sem.at[2 + l]).start()

    right, left = wrap(x + 1, 4), wrap(x - 1, 4)
    across = wrap(x + 2, 4)
    other = 1 - yl
    to_right = (z, yh, c, right, yl)
    to_left = (z, yh, c, left, yl)
    to_other = (z, yh, c, x, other)

    def rows_at(i):
        return pl.ds(pl.multiple_of(i * CHUNK, CHUNK), CHUNK)

    def upper(i):
        return pl.ds(pl.multiple_of(i * CHUNK, HALF), HALF)

    def lower(i):
        return pl.ds(pl.multiple_of(i * CHUNK + HALF, HALF), HALF)

    class Gather:
        def __init__(self, buffer, sems, sender):
            self.buffer, self.sems, self.sender = buffer, sems, sender

        def push(self, kind, slot, rows, i, device):
            ref = self.buffer.at[slot, rows]
            remote(ref, ref, self.sender, self.sems.at[kind, i], device).start()

        def wait(self, kind, slot, rows, i):
            wait_bytes(self.buffer.at[slot, rows], self.sems.at[kind, i])

        def own(self, i):
            self.push(2, mine, rows_at(i), i, to_other)
            self.push(0, mine, rows_at(i), i, to_right)
            self.push(1, mine, rows_at(i), i, to_left)

        def halves(self, i):
            self.wait(0, left * 2 + yl, rows_at(i), i)
            self.push(3, left * 2 + yl, upper(i), i, to_right)
            self.wait(1, right * 2 + yl, rows_at(i), i)
            self.push(4, right * 2 + yl, lower(i), i, to_left)

        def pair(self, i):
            self.wait(2, x * 2 + other, rows_at(i), i)
            self.push(5, x * 2 + other, rows_at(i), i, to_right)
            self.push(6, x * 2 + other, rows_at(i), i, to_left)

        def far(self, i):
            self.wait(3, across * 2 + yl, upper(i), i)
            self.wait(4, across * 2 + yl, lower(i), i)
            self.push(7, across * 2 + yl, rows_at(i), i, to_other)

        def last(self, i):
            self.wait(5, left * 2 + other, rows_at(i), i)
            self.wait(6, right * 2 + other, rows_at(i), i)
            self.wait(7, across * 2 + other, rows_at(i), i)

    def each_chunk(body):
        def step(i, carry):
            body(i)
            return carry

        lax.fori_loop(0, CHUNKS, step, 0)

    def row_scale(buffer, target, i):
        rows = rows_at(i)
        total = jnp.zeros((CHUNK, WIDTH), F32)
        for k in range(PARTS):
            value = buffer[k, rows, :].astype(F32)
            total = total + value * value
        mean = jnp.sum(total, axis=1, keepdims=True) / D
        target[rows, :] = jnp.broadcast_to(lax.rsqrt(mean + epsilon), (CHUNK, 128))

    def weight(l, k):
        return recv[2 + l, pl.ds(4 * k, 4)].reshape(WIDTH, WIDTH)

    def product(buffer, l, i):
        rows = rows_at(i)
        total = dot(buffer[0, rows, :], weight(l, 0), (1, 0))
        for k in range(1, PARTS):
            total = total + dot(buffer[k, rows, :], weight(l, k), (1, 0))
        return total

    load = [
        pltpu.make_async_copy(deltas_ref.at[0, 0], raw.at[0], load_sem.at[0]),
        pltpu.make_async_copy(deltas_ref.at[0, 1], raw.at[1], load_sem.at[1]),
        pltpu.make_async_copy(tokens_ref.at[0], tok.at[mine], load_sem.at[2]),
        pltpu.make_async_copy(cot_ref.at[0], cot, load_sem.at[3]),
        pltpu.make_async_copy(anchor_ref, anchor, load_sem.at[4]),
        pltpu.make_async_copy(momentum_ref, momentum, load_sem.at[5]),
    ]
    for copy in load:
        copy.start()

    def narrow(l):
        def one(g, carry):
            rows = pl.ds(pl.multiple_of(g * BLOCK, BLOCK), BLOCK)
            send[l, g] = raw[l, rows, :].astype(BF16)
            return carry

        lax.fori_loop(0, GROUPS, one, 0)
        recv[l, group] = send[l, group]

    tokens = Gather(tok, tok_sem, send_sem.at[8])
    states = Gather(state, state_sem, send_sem.at[9])

    load[0].wait()
    narrow(0)
    send_blocks(0)
    load[2].wait()
    each_chunk(tokens.own)
    load[1].wait()
    narrow(1)
    send_blocks(1)
    forward_blocks(0)
    each_chunk(tokens.halves)
    each_chunk(tokens.pair)
    load[4].wait()
    load[5].wait()
    update(0)
    send_blocks(2)
    forward_blocks(1)
    each_chunk(tokens.far)
    update(1)
    send_blocks(3)
    each_chunk(tokens.last)
    each_chunk(lambda i: row_scale(tok, scale0, i))
    load[3].wait()
    forward_blocks(2)
    wait_bytes(recv.at[2, pl.ds(0, GROUPS - 1)], recv_sem.at[2])

    def first(i):
        rows = rows_at(i)
        value = product(tok, 0, i) * (scale0[rows, 0:1] * FACTOR)
        pre0[rows, :] = value
        fresh = tok[mine, rows, :].astype(F32) + value * sigmoid(value)
        state[mine, rows, :] = fresh.astype(BF16)
        states.own(i)

    each_chunk(first)
    forward_blocks(3)
    each_chunk(states.halves)
    each_chunk(states.pair)
    each_chunk(states.far)
    wait_bytes(recv.at[3, pl.ds(0, GROUPS - 1)], recv_sem.at[3])

    def push(kind, src, dst, i, device):
        remote(src, dst, send_sem.at[10], rs_sem.at[kind, i], device).start()

    inner[mine] = jnp.zeros((8, CHUNK), F32)

    def second(i):
        states.last(i)
        rows = rows_at(i)
        row_scale(state, scale1, i)
        scale = scale1[rows, 0:1]
        value = product(state, 1, i) * (scale * FACTOR)
        slope = cot[rows, :].astype(F32) * silu_slope(value)
        narrow_slope = slope.astype(BF16)
        slopes[rows, :] = (slope * scale).astype(BF16)
        for k in range(PARTS):
            term = dot(narrow_slope, weight(1, k), (1, 1)) * FACTOR
            terms[k, rows, :] = term.astype(BF16)
        share = jnp.sum(slope * value, axis=1, keepdims=True)
        flat = jnp.transpose(jnp.broadcast_to(share, (CHUNK, 128)))[0:8, :]
        line = lax.broadcasted_iota(jnp.int32, (8, CHUNK), 0)
        inner[mine] = jnp.where(line == i, flat, inner[mine])
        push(0, terms.at[across * 2 + other, rows], ra.at[0, rows], i, to_other)
        push(1, terms.at[right * 2 + other, rows], ra.at[1, rows], i, to_right)
        push(2, terms.at[left * 2 + other, rows], ra.at[2, rows], i, to_left)

    each_chunk(second)
    for step in range(1, PARTS):
        there = wrap(mine + step, PARTS)
        remote(
            inner.at[mine],
            inner.at[mine],
            send_sem.at[11],
            inner_sem,
            (z, yh, c, there // 2, lax.rem(there, 2)),
        ).start()

    def grad_of(buffer, l, k):
        return dot(buffer[k], slopes[...], (0, 0)) * FACTOR

    def second_grad(k, carry):
        rows = pl.ds(pl.multiple_of(k * WIDTH, WIDTH), WIDTH)
        gout[1, rows, :] = grad_of(state, 1, k).astype(BF16)
        return carry

    def join(i):
        rows = rows_at(i)
        wait_bytes(ra.at[0, rows], rs_sem.at[0, i])
        slot = across * 2 + yl
        total = terms[slot, rows, :].astype(F32) + ra[0, rows, :].astype(F32)
        terms[slot, rows, :] = total.astype(BF16)
        push(3, terms.at[slot, upper(i)], rb.at[0, i], i, to_right)
        push(4, terms.at[slot, lower(i)], rb.at[1, i], i, to_left)

    def meet(i):
        rows = rows_at(i)
        wait_bytes(ra.at[1, rows], rs_sem.at[1, i])
        wait_bytes(ra.at[2, rows], rs_sem.at[2, i])
        slot = x * 2 + other
        total = (
            terms[slot, rows, :].astype(F32)
            + ra[1, rows, :].astype(F32)
            + ra[2, rows, :].astype(F32)
        )
        terms[slot, rows, :] = total.astype(BF16)
        push(7, terms.at[slot, rows], rc.at[2, rows], i, to_other)

    def pass_on(i):
        rows = rows_at(i)
        wait_bytes(rb.at[0, i], rs_sem.at[3, i])
        slot = right * 2 + yl
        total = terms[slot, upper(i), :].astype(F32) + rb[0, i].astype(F32)
        terms[slot, upper(i), :] = total.astype(BF16)
        push(5, terms.at[slot, rows], rc.at[0, rows], i, to_right)
        wait_bytes(rb.at[1, i], rs_sem.at[4, i])
        slot = left * 2 + yl
        total = terms[slot, lower(i), :].astype(F32) + rb[1, i].astype(F32)
        terms[slot, lower(i), :] = total.astype(BF16)
        push(6, terms.at[slot, rows], rc.at[1, rows], i, to_left)

    each_chunk(join)
    lax.fori_loop(0, PARTS, second_grad, 0)
    each_chunk(meet)
    each_chunk(pass_on)
    pltpu.make_async_copy(gout.at[1], out_grads.at[0, 1], store_sem.at[4]).start()
    wait_bytes(inner.at[pl.ds(0, PARTS - 1)], inner_sem)
    acc[...] = jnp.zeros_like(acc)

    def finish(i):
        rows = rows_at(i)
        wait_bytes(rc.at[0, rows], rs_sem.at[5, i])
        wait_bytes(rc.at[1, rows], rs_sem.at[6, i])
        wait_bytes(rc.at[2, rows], rs_sem.at[7, i])
        normed_grad = (
            terms[mine, rows, :].astype(F32)
            + rc[0, rows, :].astype(F32)
            + rc[1, rows, :].astype(F32)
            + rc[2, rows, :].astype(F32)
        )
        line = lax.broadcasted_iota(jnp.int32, (8, CHUNK), 0)
        total = inner[0]
        for k in range(1, PARTS):
            total = total + inner[k]
        flat = jnp.sum(jnp.where(line == i, total, 0.0), axis=0, keepdims=True)
        share = jnp.transpose(jnp.broadcast_to(flat, (128, CHUNK)))[:, 0:1]
        scale = scale1[rows, 0:1]
        state_grad = (
            cot[rows, :].astype(F32)
            + scale * normed_grad
            - state[mine, rows, :].astype(F32) * (scale * scale * share / D)
        )
        slope = state_grad * silu_slope(pre0[rows, :])
        narrow_slope = (slope * scale0[rows, 0:1]).astype(BF16)
        for k in range(PARTS):
            acc[k] += dot(tok[k, rows, :], narrow_slope, (0, 0))

    each_chunk(finish)

    def first_grad(k, carry):
        rows = pl.ds(pl.multiple_of(k * WIDTH, WIDTH), WIDTH)
        gout[0, rows, :] = (acc[k] * FACTOR).astype(BF16)
        return carry

    lax.fori_loop(0, PARTS, first_grad, 0)
    pltpu.make_async_copy(gout.at[0], out_grads.at[0, 0], store_sem.at[5]).start()

    for p in range(4):
        wait_bytes(send.at[p, pl.ds(0, GROUPS - 1)], send_sem.at[p])
        wait_bytes(relay.at[p], send_sem.at[4 + p])
    wait_bytes(tok.at[pl.ds(0, PARTS - 1)], send_sem.at[8])
    wait_bytes(state.at[pl.ds(0, PARTS - 1)], send_sem.at[9])
    wait_bytes(terms.at[pl.ds(0, PARTS - 1)], send_sem.at[10])
    wait_bytes(inner.at[pl.ds(0, PARTS - 1)], send_sem.at[11])
    for l in range(LEVELS):
        part = pl.ds(l * MODS, MODS)
        pltpu.make_async_copy(anchor.at[part], out_anchor.at[part], store_sem.at[l]).wait()
        pltpu.make_async_copy(momentum.at[part], out_momentum.at[part], store_sem.at[2 + l]).wait()
    pltpu.make_async_copy(gout.at[1], out_grads.at[0, 1], store_sem.at[4]).wait()
    pltpu.make_async_copy(gout.at[0], out_grads.at[0, 0], store_sem.at[5]).wait()


def shards(anchor, momentum, deltas, old_path, new_path, tokens, cotangent):
    anywhere = pl.BlockSpec(memory_space=pl.ANY)
    scalars = pl.BlockSpec(memory_space=pltpu.SMEM)
    dma = pltpu.SemaphoreType.DMA
    return pl.pallas_call(
        kernel,
        out_shape=(
            jax.ShapeDtypeStruct(anchor.shape, F32),
            jax.ShapeDtypeStruct(momentum.shape, F32),
            jax.ShapeDtypeStruct((1, LEVELS, D, WIDTH), BF16),
        ),
        in_specs=[scalars, scalars] + [anywhere] * 5,
        out_specs=(anywhere,) * 3,
        scratch_shapes=[
            pltpu.VMEM((LEVELS, D, WIDTH), F32),
            pltpu.VMEM((4, GROUPS, BLOCK, WIDTH), BF16),
            pltpu.VMEM((4, GROUPS, BLOCK, WIDTH), BF16),
            pltpu.VMEM((4, RELAYS, BLOCK, WIDTH), BF16),
            pltpu.VMEM((LEVELS * MODS, BLOCK, WIDTH), F32),
            pltpu.VMEM((LEVELS * MODS, BLOCK, WIDTH), F32),
            pltpu.VMEM((LEVELS * MODS, BLOCK, WIDTH), BF16),
            pltpu.VMEM((PARTS, ROWS, WIDTH), BF16),
            pltpu.VMEM((ROWS, WIDTH), BF16),
            pltpu.VMEM((PARTS, ROWS, WIDTH), BF16),
            pltpu.VMEM((ROWS, WIDTH), F32),
            pltpu.VMEM((ROWS, 128), F32),
            pltpu.VMEM((ROWS, 128), F32),
            pltpu.VMEM((ROWS, WIDTH), BF16),
            pltpu.VMEM((PARTS, ROWS, WIDTH), BF16),
            pltpu.VMEM((3, ROWS, WIDTH), BF16),
            pltpu.VMEM((2, CHUNKS, HALF, WIDTH), BF16),
            pltpu.VMEM((3, ROWS, WIDTH), BF16),
            pltpu.VMEM((PARTS, 8, CHUNK), F32),
            pltpu.VMEM((PARTS, WIDTH, WIDTH), F32),
            pltpu.VMEM((LEVELS, D, WIDTH), BF16),
            dma((6,)),
            dma((6,)),
            dma((12,)),
            dma((4, RELAYS)),
            dma((4,)),
            dma((8, CHUNKS)),
            dma((8, CHUNKS)),
            dma((8, CHUNKS)),
            dma(()),
        ],
        compiler_params=pltpu.CompilerParams(
            has_side_effects=True, vmem_limit_bytes=62 * 1024 * 1024
        ),
    )(old_path, new_path, anchor, momentum, deltas, tokens, cotangent)


def solution(mesh):
    split = Mesh(mesh.devices.reshape(SIZES), AXES)
    placed = (
        P(None, GROUP, MP),
        P(None, GROUP, MP),
        P(GROUP, None, None, MP),
        P(),
        P(),
        P(GROUP, None, MP),
        P(GROUP, None, MP),
    )
    return jax.shard_map(
        shards,
        mesh=split,
        in_specs=placed,
        out_specs=(P(None, GROUP, MP), P(None, GROUP, MP), P(GROUP, None, None, MP)),
        check_vma=False,
    )
```

```python
import math

import jax
import jax.numpy as jnp
from jax import lax
from jax.experimental import pallas as pl
from jax.experimental.pallas import tpu as pltpu
from jax.sharding import Mesh
from jax.sharding import PartitionSpec as P

D = 2048
MODS = 8
GROUPS = 32
ROWS = 1024
LEVELS = 2
BLOCK = D // GROUPS
WIDTH = 256
PARTS = D // WIDTH
CHUNKS = 4
CHUNK = ROWS // CHUNKS
HALF = CHUNK // 2
TILE = 16
SPAN = 8
FACTOR = 1.0 / math.sqrt(D)

outer_rate = 0.7
momentum_rate = 0.9
epsilon = 1e-06

AXES = ("z", "yh", "c", "x", "yl")
SIZES = (8, 2, 2, 4, 2)
GROUP = ("z", "yh", "c")
MP = ("x", "yl")
NEAR = (3, -3, 2, -2, 1, -1, 0)
RELAYS = 18
BF16 = jnp.bfloat16
F32 = jnp.float32


def wrap(value, size):
    return lax.rem(value + size, size)


def sigmoid(values):
    return 1.0 / (1.0 + jnp.exp(-values))


def silu_slope(values):
    part = sigmoid(values)
    return part * (1.0 + values * (1.0 - part))


def dot(a, b, dims):
    return lax.dot_general(a, b, ((dims[0:1], dims[1:2]), ((), ())), preferred_element_type=F32)


def kernel(
    old_ref,
    new_ref,
    anchor_ref,
    momentum_ref,
    deltas_ref,
    tokens_ref,
    cot_ref,
    anchor,
    momentum,
    grads,
    raw,
    send,
    recv,
    relay,
    modules,
    tok,
    cot,
    state,
    pre0,
    scale0,
    scale1,
    slopes,
    terms,
    ra,
    rb,
    rc,
    inner,
    acc,
    load_sem,
    send_sem,
    relay_sem,
    recv_sem,
    tok_sem,
    state_sem,
    rs_sem,
    inner_sem,
):
    z = lax.axis_index("z")
    yh = lax.axis_index("yh")
    c = lax.axis_index("c")
    x = lax.axis_index("x")
    yl = lax.axis_index("yl")
    y = yh * 2 + yl
    group = z * 4 + yh * 2 + c
    mine = x * 2 + yl

    def remote(src, dst, sender, receiver, device):
        return pltpu.make_async_remote_copy(
            src_ref=src,
            dst_ref=dst,
            send_sem=sender,
            recv_sem=receiver,
            device_id=device,
            device_id_type=pl.DeviceIdType.MESH,
        )

    def wait_bytes(ref, sem):
        pltpu.make_async_copy(ref, ref, sem).wait()

    def place(dz, dy, core):
        there = wrap(y + dy, 4)
        return (wrap(z + dz, 8), there // 2, core, x, lax.rem(there, 2))

    partners = [place(0, 0, 1 - c)]
    for dz in NEAR:
        if dz != 0:
            partners += [place(dz, 0, 0), place(dz, 0, 1)]
        for dy in (1, -1):
            partners.append(place(dz, dy, c))
            if dz in (0, 2, -2):
                partners.append(place(dz, dy, 1 - c))
    for dx in (1, 2, 3):
        for part in (yl, 1 - yl):
            partners.append((z, yh, c, wrap(x + dx, 4), part))
    barrier = pltpu.get_barrier_semaphore()
    for partner in partners:
        pl.semaphore_signal(
            barrier, inc=1, device_id=partner, device_id_type=pl.DeviceIdType.MESH
        )

    def send_block(p, dz, cross, core, dst, receiver, device):
        target = wrap(z + dz, 8) * 4 + lax.rem(yh + cross, 2) * 2 + core
        remote(send.at[p, target], dst, send_sem.at[p], receiver, device).start()

    def send_relayed(p):
        def go(dz, cross, core, slot, device):
            send_block(p, dz, cross, core, relay.at[p, slot], relay_sem.at[p, slot], device)

        for i, sign in enumerate((1, -1)):
            go(4, 1, i, 14 + i, place(2 * sign, sign, c))
            go(4, 0, i, 16 + i, place(2 * sign, 0, c))
        for j, dz in enumerate(NEAR):
            for i, sign in enumerate((1, -1)):
                go(dz, 1, i, i * 7 + j, place(dz, sign, c))

    def send_direct(p):
        for dz in NEAR:
            for core in (1 - c,) if dz == 0 else (0, 1):
                device = place(dz, 0, core)
                send_block(p, dz, 0, core, recv.at[p, group], recv_sem.at[p], device)

    def forward_blocks(p):
        def go(slot, dz, dy, device):
            source = wrap(z - dz, 8) * 4 + (wrap(y - dy, 4) // 2) * 2 + c
            wait_bytes(relay.at[p, slot], relay_sem.at[p, slot])
            remote(
                relay.at[p, slot], recv.at[p, source], send_sem.at[4 + p], recv_sem.at[p], device
            ).start()

        for i, sign in enumerate((1, -1)):
            go(14 + i, 2 * sign, sign, place(2 * sign, sign, i))
            go(16 + i, 2 * sign, 0, place(2 * sign, 0, i))
        for j, dz in enumerate(NEAR):
            for i, sign in enumerate((1, -1)):
                go(i * 7 + j, dz, sign, place(0, sign, i))

    def update(l):
        wait_bytes(recv.at[l, pl.ds(0, GROUPS - 1)], recv_sem.at[l])

        def count_one(g, counts):
            named = old_ref[l, g]
            return tuple(n + jnp.where(named == m, 1.0, 0.0) for m, n in enumerate(counts))

        counts = lax.fori_loop(0, GROUPS, count_one, (jnp.float32(0.0),) * MODS)

        def rows_of(r, carry):
            rows = pl.ds(pl.multiple_of(r * TILE, TILE), TILE)

            def add_some(step, sums):
                for j in range(SPAN):
                    g = step * SPAN + j
                    named = old_ref[l, g]
                    value = recv[l, g, rows, :].astype(F32)
                    sums = tuple(
                        s + value * jnp.where(named == m, 1.0, 0.0) for m, s in enumerate(sums)
                    )
                return sums

            sums = lax.fori_loop(
                0, GROUPS // SPAN, add_some, (jnp.zeros((TILE, WIDTH), F32),) * MODS
            )
            for m in range(MODS):
                k = l * MODS + m
                outer_grad = sums[m] / counts[m]
                fresh = momentum_rate * momentum[k, rows, :] + outer_grad
                moved = anchor[k, rows, :] - outer_rate * (outer_grad + momentum_rate * fresh)
                momentum[k, rows, :] = fresh
                anchor[k, rows, :] = moved
                modules[k, rows, :] = moved.astype(BF16)
            return carry

        lax.fori_loop(0, BLOCK // TILE, rows_of, 0)

        def stage(g, carry):
            send[2 + l, g] = modules[l * MODS + new_ref[l, g]]
            return carry

        lax.fori_loop(0, GROUPS, stage, 0)
        recv[2 + l, group] = modules[l * MODS + new_ref[l, group]]

    right, left = wrap(x + 1, 4), wrap(x - 1, 4)
    across = wrap(x + 2, 4)
    other = 1 - yl
    to_right = (z, yh, c, right, yl)
    to_left = (z, yh, c, left, yl)
    to_other = (z, yh, c, x, other)

    def rows_at(i):
        return pl.ds(pl.multiple_of(i * CHUNK, CHUNK), CHUNK)

    def upper(i):
        return pl.ds(pl.multiple_of(i * CHUNK, HALF), HALF)

    def lower(i):
        return pl.ds(pl.multiple_of(i * CHUNK + HALF, HALF), HALF)

    class Gather:
        def __init__(self, buffer, sems, sender):
            self.buffer, self.sems, self.sender = buffer, sems, sender

        def push(self, kind, slot, rows, i, device):
            ref = self.buffer.at[slot, rows]
            remote(ref, ref, self.sender, self.sems.at[kind, i], device).start()

        def wait(self, kind, slot, rows, i):
            wait_bytes(self.buffer.at[slot, rows], self.sems.at[kind, i])

        def own(self, i):
            self.push(2, mine, rows_at(i), i, to_other)
            self.push(0, mine, rows_at(i), i, to_right)
            self.push(1, mine, rows_at(i), i, to_left)

        def halves(self, i):
            self.wait(0, left * 2 + yl, rows_at(i), i)
            self.push(3, left * 2 + yl, upper(i), i, to_right)
            self.wait(1, right * 2 + yl, rows_at(i), i)
            self.push(4, right * 2 + yl, lower(i), i, to_left)

        def pair(self, i):
            self.wait(2, x * 2 + other, rows_at(i), i)
            self.push(5, x * 2 + other, rows_at(i), i, to_right)
            self.push(6, x * 2 + other, rows_at(i), i, to_left)

        def far(self, i):
            self.wait(3, across * 2 + yl, upper(i), i)
            self.wait(4, across * 2 + yl, lower(i), i)
            self.push(7, across * 2 + yl, rows_at(i), i, to_other)

        def last(self, i):
            self.wait(5, left * 2 + other, rows_at(i), i)
            self.wait(6, right * 2 + other, rows_at(i), i)
            self.wait(7, across * 2 + other, rows_at(i), i)

    def each_chunk(body):
        def step(i, carry):
            body(i)
            return carry

        lax.fori_loop(0, CHUNKS, step, 0)

    def row_scale(buffer, target, i):
        rows = rows_at(i)
        total = jnp.zeros((CHUNK, WIDTH), F32)
        for k in range(PARTS):
            value = buffer[k, rows, :].astype(F32)
            total = total + value * value
        mean = jnp.sum(total, axis=1, keepdims=True) / D
        target[rows, :] = jnp.broadcast_to(lax.rsqrt(mean + epsilon), (CHUNK, 128))

    def weight(l, k):
        return recv[2 + l, pl.ds(4 * k, 4)].reshape(WIDTH, WIDTH)

    def product(buffer, l, i):
        rows = rows_at(i)
        total = dot(buffer[0, rows, :], weight(l, 0), (1, 0))
        for k in range(1, PARTS):
            total = total + dot(buffer[k, rows, :], weight(l, k), (1, 0))
        return total

    load = [
        pltpu.make_async_copy(deltas_ref.at[0, 0], raw.at[0], load_sem.at[0]),
        pltpu.make_async_copy(deltas_ref.at[0, 1], raw.at[1], load_sem.at[1]),
        pltpu.make_async_copy(tokens_ref.at[0], tok.at[mine], load_sem.at[2]),
        pltpu.make_async_copy(cot_ref.at[0], cot, load_sem.at[3]),
        pltpu.make_async_copy(anchor_ref, anchor, load_sem.at[4]),
        pltpu.make_async_copy(momentum_ref, momentum, load_sem.at[5]),
    ]
    for copy in load:
        copy.start()

    def narrow(l):
        def one(g, carry):
            rows = pl.ds(pl.multiple_of(g * BLOCK, BLOCK), BLOCK)
            send[l, g] = raw[l, rows, :].astype(BF16)
            return carry

        lax.fori_loop(0, GROUPS, one, 0)
        recv[l, group] = send[l, group]

    tokens = Gather(tok, tok_sem, send_sem.at[8])
    states = Gather(state, state_sem, send_sem.at[9])

    load[0].wait()
    narrow(0)
    pl.semaphore_wait(barrier, len(partners))
    send_relayed(0)
    send_direct(0)
    load[2].wait()
    each_chunk(tokens.own)
    load[1].wait()
    narrow(1)
    forward_blocks(0)
    send_relayed(1)
    each_chunk(tokens.halves)
    each_chunk(tokens.pair)
    each_chunk(tokens.far)
    load[4].wait()
    load[5].wait()
    update(0)
    send_relayed(2)
    send_direct(2)
    forward_blocks(1)
    forward_blocks(2)
    send_direct(1)
    each_chunk(tokens.last)
    each_chunk(lambda i: row_scale(tok, scale0, i))
    load[3].wait()
    wait_bytes(recv.at[2, pl.ds(0, GROUPS - 1)], recv_sem.at[2])

    def first(i):
        rows = rows_at(i)
        value = product(tok, 0, i) * (scale0[rows, 0:1] * FACTOR)
        pre0[rows, :] = value
        fresh = tok[mine, rows, :].astype(F32) + value * sigmoid(value)
        state[mine, rows, :] = fresh.astype(BF16)
        states.own(i)

    each_chunk(first)
    update(1)
    send_relayed(3)
    send_direct(3)
    each_chunk(states.halves)
    each_chunk(states.pair)
    each_chunk(states.far)
    forward_blocks(3)

    def gathered(i):
        states.last(i)
        row_scale(state, scale1, i)

    each_chunk(gathered)
    wait_bytes(recv.at[3, pl.ds(0, GROUPS - 1)], recv_sem.at[3])

    def push(kind, src, dst, i, device):
        remote(src, dst, send_sem.at[10], rs_sem.at[kind, i], device).start()

    inner[mine] = jnp.zeros((8, CHUNK), F32)

    def second(i):
        rows = rows_at(i)
        scale = scale1[rows, 0:1]
        value = product(state, 1, i) * (scale * FACTOR)
        slope = cot[rows, :].astype(F32) * silu_slope(value)
        narrow_slope = slope.astype(BF16)

        def term(slot):
            product_of = dot(narrow_slope, weight(1, slot), (1, 1)) * FACTOR
            terms[slot, rows, :] = product_of.astype(BF16)

        outgoing = (
            (across * 2 + other, to_other),
            (right * 2 + other, to_right),
            (left * 2 + other, to_left),
        )
        for kind, (slot, device) in enumerate(outgoing):
            term(slot)
        for kind, (slot, device) in enumerate(outgoing):
            push(kind, terms.at[slot, rows], ra.at[kind, rows], i, device)
        for slot in (across * 2 + yl, x * 2 + other, right * 2 + yl, left * 2 + yl, mine):
            term(slot)
        slopes[rows, :] = (slope * scale).astype(BF16)
        share = jnp.sum(slope * value, axis=1, keepdims=True)
        flat = jnp.transpose(jnp.broadcast_to(share, (CHUNK, 128)))[0:8, :]
        line = lax.broadcasted_iota(jnp.int32, (8, CHUNK), 0)
        inner[mine] = jnp.where(line == i, flat, inner[mine])

    each_chunk(second)
    for step in range(1, PARTS):
        there = wrap(mine + step, PARTS)
        remote(
            inner.at[mine],
            inner.at[mine],
            send_sem.at[11],
            inner_sem,
            (z, yh, c, there // 2, lax.rem(there, 2)),
        ).start()

    def grad_of(buffer, l, k):
        return dot(buffer[k], slopes[...], (0, 0)) * FACTOR

    def second_grad(k, carry):
        rows = pl.ds(pl.multiple_of(k * WIDTH, WIDTH), WIDTH)
        grads[0, 1, rows, :] = grad_of(state, 1, k).astype(BF16)
        return carry

    def join(i):
        rows = rows_at(i)
        wait_bytes(ra.at[0, rows], rs_sem.at[0, i])
        slot = across * 2 + yl
        total = terms[slot, rows, :].astype(F32) + ra[0, rows, :].astype(F32)
        terms[slot, rows, :] = total.astype(BF16)
        push(3, terms.at[slot, upper(i)], rb.at[0, i], i, to_right)
        push(4, terms.at[slot, lower(i)], rb.at[1, i], i, to_left)

    def meet(i):
        rows = rows_at(i)
        wait_bytes(ra.at[1, rows], rs_sem.at[1, i])
        wait_bytes(ra.at[2, rows], rs_sem.at[2, i])
        slot = x * 2 + other
        total = (
            terms[slot, rows, :].astype(F32)
            + ra[1, rows, :].astype(F32)
            + ra[2, rows, :].astype(F32)
        )
        terms[slot, rows, :] = total.astype(BF16)
        push(7, terms.at[slot, rows], rc.at[2, rows], i, to_other)

    def pass_on(i):
        rows = rows_at(i)
        wait_bytes(rb.at[0, i], rs_sem.at[3, i])
        slot = right * 2 + yl
        total = terms[slot, upper(i), :].astype(F32) + rb[0, i].astype(F32)
        terms[slot, upper(i), :] = total.astype(BF16)
        push(5, terms.at[slot, rows], rc.at[0, rows], i, to_right)
        wait_bytes(rb.at[1, i], rs_sem.at[4, i])
        slot = left * 2 + yl
        total = terms[slot, lower(i), :].astype(F32) + rb[1, i].astype(F32)
        terms[slot, lower(i), :] = total.astype(BF16)
        push(6, terms.at[slot, rows], rc.at[1, rows], i, to_left)

    each_chunk(join)
    lax.fori_loop(0, PARTS, second_grad, 0)
    each_chunk(meet)
    each_chunk(pass_on)
    wait_bytes(inner.at[pl.ds(0, PARTS - 1)], inner_sem)
    acc[...] = jnp.zeros_like(acc)

    def finish(i):
        rows = rows_at(i)
        wait_bytes(rc.at[0, rows], rs_sem.at[5, i])
        wait_bytes(rc.at[1, rows], rs_sem.at[6, i])
        wait_bytes(rc.at[2, rows], rs_sem.at[7, i])
        normed_grad = (
            terms[mine, rows, :].astype(F32)
            + rc[0, rows, :].astype(F32)
            + rc[1, rows, :].astype(F32)
            + rc[2, rows, :].astype(F32)
        )
        line = lax.broadcasted_iota(jnp.int32, (8, CHUNK), 0)
        total = inner[0]
        for k in range(1, PARTS):
            total = total + inner[k]
        flat = jnp.sum(jnp.where(line == i, total, 0.0), axis=0, keepdims=True)
        share = jnp.transpose(jnp.broadcast_to(flat, (128, CHUNK)))[:, 0:1]
        scale = scale1[rows, 0:1]
        state_grad = (
            cot[rows, :].astype(F32)
            + scale * normed_grad
            - state[mine, rows, :].astype(F32) * (scale * scale * share / D)
        )
        slope = state_grad * silu_slope(pre0[rows, :])
        narrow_slope = (slope * scale0[rows, 0:1]).astype(BF16)
        for k in range(PARTS):
            acc[k] += dot(tok[k, rows, :], narrow_slope, (0, 0))

    each_chunk(finish)

    def first_grad(k, carry):
        rows = pl.ds(pl.multiple_of(k * WIDTH, WIDTH), WIDTH)
        grads[0, 0, rows, :] = (acc[k] * FACTOR).astype(BF16)
        return carry

    lax.fori_loop(0, PARTS, first_grad, 0)

    for p in range(4):
        wait_bytes(send.at[p, pl.ds(0, GROUPS - 1)], send_sem.at[p])
        wait_bytes(relay.at[p], send_sem.at[4 + p])
    wait_bytes(tok.at[pl.ds(0, PARTS - 1)], send_sem.at[8])
    wait_bytes(state.at[pl.ds(0, PARTS - 1)], send_sem.at[9])
    wait_bytes(terms.at[pl.ds(0, PARTS - 1)], send_sem.at[10])
    wait_bytes(inner.at[pl.ds(0, PARTS - 1)], send_sem.at[11])


def shards(anchor, momentum, deltas, old_path, new_path, tokens, cotangent):
    anywhere = pl.BlockSpec(memory_space=pltpu.HBM)
    scalars = pl.BlockSpec(memory_space=pltpu.SMEM)
    dma = pltpu.SemaphoreType.DMA
    return pl.pallas_call(
        kernel,
        out_shape=(
            pltpu.VMEM(anchor.shape, F32),
            pltpu.VMEM(momentum.shape, F32),
            pltpu.VMEM((1, LEVELS, D, WIDTH), BF16),
        ),
        in_specs=[scalars, scalars] + [anywhere] * 5,
        out_specs=(pl.BlockSpec(memory_space=pltpu.VMEM),) * 3,
        scratch_shapes=[
            pltpu.VMEM((LEVELS, D, WIDTH), F32),
            pltpu.VMEM((4, GROUPS, BLOCK, WIDTH), BF16),
            pltpu.VMEM((4, GROUPS, BLOCK, WIDTH), BF16),
            pltpu.VMEM((4, RELAYS, BLOCK, WIDTH), BF16),
            pltpu.VMEM((LEVELS * MODS, BLOCK, WIDTH), BF16),
            pltpu.VMEM((PARTS, ROWS, WIDTH), BF16),
            pltpu.VMEM((ROWS, WIDTH), BF16),
            pltpu.VMEM((PARTS, ROWS, WIDTH), BF16),
            pltpu.VMEM((ROWS, WIDTH), F32),
            pltpu.VMEM((ROWS, 128), F32),
            pltpu.VMEM((ROWS, 128), F32),
            pltpu.VMEM((ROWS, WIDTH), BF16),
            pltpu.VMEM((PARTS, ROWS, WIDTH), BF16),
            pltpu.VMEM((3, ROWS, WIDTH), BF16),
            pltpu.VMEM((2, CHUNKS, HALF, WIDTH), BF16),
            pltpu.VMEM((3, ROWS, WIDTH), BF16),
            pltpu.VMEM((PARTS, 8, CHUNK), F32),
            pltpu.VMEM((PARTS, WIDTH, WIDTH), F32),
            dma((6,)),
            dma((12,)),
            dma((4, RELAYS)),
            dma((4,)),
            dma((8, CHUNKS)),
            dma((8, CHUNKS)),
            dma((8, CHUNKS)),
            dma(()),
        ],
        compiler_params=pltpu.CompilerParams(
            collective_id=0, has_side_effects=True, vmem_limit_bytes=59 * 1024 * 1024
        ),
    )(old_path.T, new_path.T, anchor, momentum, deltas, tokens, cotangent)


def solution(mesh):
    split = Mesh(mesh.devices.reshape(SIZES), AXES)
    placed = (
        P(None, GROUP, MP),
        P(None, GROUP, MP),
        P(GROUP, None, None, MP),
        P(),
        P(),
        P(GROUP, None, MP),
        P(GROUP, None, MP),
    )
    return jax.shard_map(
        shards,
        mesh=split,
        in_specs=placed,
        out_specs=(P(None, GROUP, MP), P(None, GROUP, MP), P(GROUP, None, None, MP)),
        check_vma=False,
    )
```

```python
import math

import jax
import jax.numpy as jnp
from jax import lax
from jax.experimental import pallas as pl
from jax.experimental.pallas import tpu as pltpu
from jax.sharding import Mesh
from jax.sharding import PartitionSpec as P

D = 2048
MODS = 8
GROUPS = 32
ROWS = 1024
LEVELS = 2
BLOCK = D // GROUPS
WIDTH = 256
PARTS = D // WIDTH
CHUNKS = 4
CHUNK = ROWS // CHUNKS
HALF = CHUNK // 2
TILE = 16
PIECE = BLOCK // 2
SPLIT = 1
FACTOR = 1.0 / math.sqrt(D)

outer_rate = 0.7
momentum_rate = 0.9
epsilon = 1e-06

AXES = ("z", "yh", "c", "x", "yl")
SIZES = (8, 2, 2, 4, 2)
GROUP = ("z", "yh", "c")
MP = ("x", "yl")
NEAR = (3, -3, 2, -2, 1, -1, 0)
RELAYS = 18
BF16 = jnp.bfloat16
F32 = jnp.float32


def wrap(value, size):
    return lax.rem(value + size, size)


def sigmoid(values):
    return 1.0 / (1.0 + jnp.exp(-values))


def silu_slope(values):
    part = sigmoid(values)
    return part * (1.0 + values * (1.0 - part))


def dot(a, b, dims):
    return lax.dot_general(a, b, ((dims[0:1], dims[1:2]), ((), ())), preferred_element_type=F32)


def kernel(
    old_table,
    new_table,
    anchor_ref,
    momentum_ref,
    deltas_ref,
    tokens_ref,
    cot_ref,
    anchor,
    momentum,
    grads,
    old_ref,
    new_ref,
    raw,
    send,
    recv,
    relay,
    modules,
    selector,
    count,
    tok,
    cot,
    state,
    pre0,
    scale0,
    scale1,
    slopes,
    terms,
    ra,
    rb,
    rc,
    inner,
    acc,
    load_sem,
    send_sem,
    relay_sem,
    recv_sem,
    tok_sem,
    state_sem,
    rs_sem,
    inner_sem,
):
    z = lax.axis_index("z")
    yh = lax.axis_index("yh")
    c = lax.axis_index("c")
    x = lax.axis_index("x")
    yl = lax.axis_index("yl")
    y = yh * 2 + yl
    group = z * 4 + yh * 2 + c
    mine = x * 2 + yl

    load = [
        pltpu.make_async_copy(deltas_ref.at[0, 0], raw.at[0], load_sem.at[0]),
        pltpu.make_async_copy(deltas_ref.at[0, 1], raw.at[1], load_sem.at[1]),
        pltpu.make_async_copy(tokens_ref.at[0], tok.at[mine], load_sem.at[2]),
        pltpu.make_async_copy(cot_ref.at[0], cot, load_sem.at[3]),
        pltpu.make_async_copy(anchor_ref, anchor, load_sem.at[4]),
        pltpu.make_async_copy(momentum_ref, momentum, load_sem.at[5]),
        pltpu.make_async_copy(old_table, old_ref, load_sem.at[6]),
        pltpu.make_async_copy(new_table, new_ref, load_sem.at[7]),
    ]
    for copy in load:
        copy.start()

    def remote(src, dst, sender, receiver, device):
        return pltpu.make_async_remote_copy(
            src_ref=src,
            dst_ref=dst,
            send_sem=sender,
            recv_sem=receiver,
            device_id=device,
            device_id_type=pl.DeviceIdType.MESH,
        )

    def wait_bytes(ref, sem):
        pltpu.make_async_copy(ref, ref, sem).wait()

    def place(dz, dy, core):
        there = wrap(y + dy, 4)
        return (wrap(z + dz, 8), there // 2, core, x, lax.rem(there, 2))

    partners = [place(0, 0, 1 - c)]
    for dz in NEAR:
        if dz != 0:
            partners += [place(dz, 0, 0), place(dz, 0, 1)]
        for dy in (1, -1):
            partners.append(place(dz, dy, c))
            if dz in (0, 2, -2):
                partners.append(place(dz, dy, 1 - c))
    for dx in (1, 2, 3):
        for part in (yl, 1 - yl):
            partners.append((z, yh, c, wrap(x + dx, 4), part))
    barrier = pltpu.get_barrier_semaphore()
    for partner in partners:
        pl.semaphore_signal(
            barrier, inc=1, device_id=partner, device_id_type=pl.DeviceIdType.MESH
        )

    def piece(h):
        return pl.ds(0, BLOCK) if h is None else pl.ds(h * PIECE, PIECE)

    def send_block(p, h, dz, cross, core, dst, receiver, device):
        target = wrap(z + dz, 8) * 4 + lax.rem(yh + cross, 2) * 2 + core
        remote(send.at[p, target, piece(h)], dst, send_sem.at[p], receiver, device).start()

    def send_relayed(p, h=None):
        def go(dz, cross, core, slot, device):
            dst, receiver = relay.at[p, slot, piece(h)], relay_sem.at[p, h or 0, slot]
            send_block(p, h, dz, cross, core, dst, receiver, device)

        for i, sign in enumerate((1, -1)):
            go(4, 1, i, 14 + i, place(2 * sign, sign, c))
            go(4, 0, i, 16 + i, place(2 * sign, 0, c))
        for j, dz in enumerate(NEAR):
            for i, sign in enumerate((1, -1)):
                go(dz, 1, i, i * 7 + j, place(dz, sign, c))

    def send_direct(p, h=None):
        for dz in NEAR:
            for core in (1 - c,) if dz == 0 else (0, 1):
                dst, receiver = recv.at[p, group, piece(h)], recv_sem.at[p, 1 + (h or 0)]
                send_block(p, h, dz, 0, core, dst, receiver, place(dz, 0, core))

    def forward_blocks(p, h=None):
        def go(slot, dz, dy, device):
            source = wrap(z - dz, 8) * 4 + (wrap(y - dy, 4) // 2) * 2 + c
            held = relay.at[p, slot, piece(h)]
            wait_bytes(held, relay_sem.at[p, h or 0, slot])
            dst = recv.at[p, source, piece(h)]
            remote(held, dst, send_sem.at[4 + p], recv_sem.at[p, 0], device).start()

        for i, sign in enumerate((1, -1)):
            go(14 + i, 2 * sign, sign, place(2 * sign, sign, i))
            go(16 + i, 2 * sign, 0, place(2 * sign, 0, i))
        for j, dz in enumerate(NEAR):
            for i, sign in enumerate((1, -1)):
                go(i * 7 + j, dz, sign, place(0, sign, i))

    def arrive_relayed(p):
        wait_bytes(recv.at[p, pl.ds(0, RELAYS)], recv_sem.at[p, 0])

    def arrive_direct(p, h=None):
        near = pl.ds(0, GROUPS - 1 - RELAYS)
        wait_bytes(recv.at[p, near, piece(h)], recv_sem.at[p, 1 + (h or 0)])

    def prepare(l):
        tall = (MODS * TILE, GROUPS * TILE)
        line = lax.broadcasted_iota(jnp.int32, tall, 0)
        lane = lax.broadcasted_iota(jnp.int32, tall, 1)
        owner = lax.broadcasted_iota(jnp.int32, (8, GROUPS * TILE), 1) // TILE
        named = jnp.zeros((8, GROUPS * TILE), jnp.int32)
        for g in range(GROUPS):
            named = jnp.where(owner == g, old_ref[l, g], named)
        wanted = jnp.broadcast_to(named[0:1, :] * TILE, tall) + lane % TILE
        chosen = jnp.where(line == wanted, 1.0, 0.0)
        selector[l] = chosen.astype(BF16)
        count[l] = jnp.broadcast_to(jnp.sum(chosen, axis=1, keepdims=True), (MODS * TILE, 128))

    def update(l, h=None):
        for r in range(BLOCK // TILE) if h is None else range(2 * h, 2 * h + 2):
            rows = pl.ds(r * TILE, TILE)
            values = recv[l, :, rows, :].reshape(GROUPS * TILE, WIDTH)
            sums = dot(selector[l], values, (1, 0)) / count[l][:, 0:1]
            for m in range(MODS):
                k = l * MODS + m
                outer_grad = sums[m * TILE : (m + 1) * TILE]
                fresh = momentum_rate * momentum[k, rows, :] + outer_grad
                moved = anchor[k, rows, :] - outer_rate * (outer_grad + momentum_rate * fresh)
                momentum[k, rows, :] = fresh
                anchor[k, rows, :] = moved
                modules[k, rows, :] = moved.astype(BF16)

        def stage(g, carry):
            send[2 + l, g, piece(h), :] = modules[l * MODS + new_ref[l, g], piece(h), :]
            return carry

        lax.fori_loop(0, GROUPS, stage, 0, unroll=4)
        recv[2 + l, group, piece(h), :] = modules[l * MODS + new_ref[l, group], piece(h), :]

    right, left = wrap(x + 1, 4), wrap(x - 1, 4)
    across = wrap(x + 2, 4)
    other = 1 - yl
    to_right = (z, yh, c, right, yl)
    to_left = (z, yh, c, left, yl)
    to_other = (z, yh, c, x, other)

    def rows_at(i):
        return pl.ds(pl.multiple_of(i * CHUNK, CHUNK), CHUNK)

    def upper(i):
        return pl.ds(pl.multiple_of(i * CHUNK, HALF), HALF)

    def lower(i):
        return pl.ds(pl.multiple_of(i * CHUNK + HALF, HALF), HALF)

    class Gather:
        def __init__(self, buffer, sems, sender):
            self.buffer, self.sems, self.sender = buffer, sems, sender

        def push(self, kind, slot, rows, i, device):
            ref = self.buffer.at[slot, rows]
            remote(ref, ref, self.sender, self.sems.at[kind, i], device).start()

        def wait(self, kind, slot, rows, i):
            wait_bytes(self.buffer.at[slot, rows], self.sems.at[kind, i])

        def own(self, i):
            self.push(2, mine, rows_at(i), i, to_other)
            self.push(0, mine, rows_at(i), i, to_right)
            self.push(1, mine, rows_at(i), i, to_left)

        def halves(self, i):
            self.wait(0, left * 2 + yl, rows_at(i), i)
            self.push(3, left * 2 + yl, upper(i), i, to_right)
            self.wait(1, right * 2 + yl, rows_at(i), i)
            self.push(4, right * 2 + yl, lower(i), i, to_left)

        def pair(self, i):
            self.wait(2, x * 2 + other, rows_at(i), i)
            self.push(5, x * 2 + other, rows_at(i), i, to_right)
            self.push(6, x * 2 + other, rows_at(i), i, to_left)

        def far(self, i):
            self.wait(3, across * 2 + yl, upper(i), i)
            self.wait(4, across * 2 + yl, lower(i), i)
            self.push(7, across * 2 + yl, rows_at(i), i, to_other)

        def far_halves(self, i):
            self.wait(5, left * 2 + other, rows_at(i), i)
            self.push(7, left * 2 + other, upper(i), i, to_right)
            self.wait(6, right * 2 + other, rows_at(i), i)
            self.push(8, right * 2 + other, lower(i), i, to_left)

        def last_halves(self, i):
            self.wait(3, across * 2 + yl, upper(i), i)
            self.wait(4, across * 2 + yl, lower(i), i)
            self.wait(7, across * 2 + other, upper(i), i)
            self.wait(8, across * 2 + other, lower(i), i)

        def last(self, i):
            self.wait(5, left * 2 + other, rows_at(i), i)
            self.wait(6, right * 2 + other, rows_at(i), i)
            self.wait(7, across * 2 + other, rows_at(i), i)

    def each_chunk(body):
        def step(i, carry):
            body(i)
            return carry

        lax.fori_loop(0, CHUNKS, step, 0)

    def row_scale(buffer, target, i):
        rows = rows_at(i)
        total = jnp.zeros((CHUNK, WIDTH), F32)
        for k in range(PARTS):
            value = buffer[k, rows, :].astype(F32)
            total = total + value * value
        mean = jnp.sum(total, axis=1, keepdims=True) / D
        target[rows, :] = jnp.broadcast_to(lax.rsqrt(mean + epsilon), (CHUNK, 128))

    def weight(l, k):
        return recv[2 + l, pl.ds(4 * k, 4)].reshape(WIDTH, WIDTH)

    def product(buffer, l, i):
        rows = rows_at(i)
        total = dot(buffer[0, rows, :], weight(l, 0), (1, 0))
        for k in range(1, PARTS):
            total = total + dot(buffer[k, rows, :], weight(l, k), (1, 0))
        return total

    def narrow(l):
        def one(g, carry):
            rows = pl.ds(pl.multiple_of(g * BLOCK, BLOCK), BLOCK)
            send[l, g] = raw[l, rows, :].astype(BF16)
            return carry

        lax.fori_loop(0, GROUPS, one, 0)
        recv[l, group] = send[l, group]

    tokens = Gather(tok, tok_sem, send_sem.at[8])
    states = Gather(state, state_sem, send_sem.at[9])

    load[0].wait()
    narrow(0)
    pl.semaphore_wait(barrier, len(partners))
    send_relayed(0)
    send_direct(0)
    load[2].wait()
    each_chunk(tokens.own)
    load[1].wait()
    narrow(1)
    load[6].wait()
    load[7].wait()
    prepare(0)
    prepare(1)
    load[4].wait()
    load[5].wait()
    forward_blocks(0)
    send_relayed(1)
    each_chunk(tokens.halves)
    each_chunk(tokens.pair)
    arrive_relayed(0)
    arrive_direct(0)
    update(0)
    send_relayed(2)
    send_direct(2)
    forward_blocks(1)
    forward_blocks(2)
    send_direct(1, 0)
    send_direct(1, 1)
    each_chunk(tokens.far_halves)
    each_chunk(tokens.last_halves)
    each_chunk(lambda i: row_scale(tok, scale0, i))
    load[3].wait()
    arrive_relayed(2)
    arrive_direct(2)

    def first(i):
        rows = rows_at(i)
        value = product(tok, 0, i) * (scale0[rows, 0:1] * FACTOR)
        pre0[rows, :] = value
        fresh = tok[mine, rows, :].astype(F32) + value * sigmoid(value)
        state[mine, rows, :] = fresh.astype(BF16)
        states.own(i)

    each_chunk(first)
    arrive_relayed(1)
    arrive_direct(1, 0)
    update(1, 0)
    send_relayed(3, 0)
    send_direct(3, 0)
    arrive_direct(1, 1)
    update(1, 1)
    send_relayed(3, 1)
    send_direct(3, 1)
    each_chunk(states.halves)
    forward_blocks(3, 0)
    each_chunk(states.pair)
    states.far(1)
    forward_blocks(3, 1)
    states.far(2)
    states.far(3)
    states.far_halves(0)
    for i in range(CHUNKS):
        if i < SPLIT:
            states.last_halves(i)
        else:
            states.last(i)
    each_chunk(lambda i: row_scale(state, scale1, i))
    arrive_relayed(3)
    arrive_direct(3, 0)
    arrive_direct(3, 1)

    def push(kind, src, dst, i, device):
        remote(src, dst, send_sem.at[10], rs_sem.at[kind, i], device).start()

    inner[mine] = jnp.zeros((8, CHUNK), F32)

    def second(i):
        rows = rows_at(i)
        scale = scale1[rows, 0:1]
        value = product(state, 1, i) * (scale * FACTOR)
        slope = cot[rows, :].astype(F32) * silu_slope(value)
        narrow_slope = slope.astype(BF16)

        def term(slot):
            product_of = dot(narrow_slope, weight(1, slot), (1, 1)) * FACTOR
            terms[slot, rows, :] = product_of.astype(BF16)

        outgoing = (
            (across * 2 + other, to_other),
            (right * 2 + other, to_right),
            (left * 2 + other, to_left),
        )
        for kind, (slot, device) in enumerate(outgoing):
            term(slot)
        for kind, (slot, device) in enumerate(outgoing):
            push(kind, terms.at[slot, rows], ra.at[kind, rows], i, device)
        for slot in (across * 2 + yl, x * 2 + other, right * 2 + yl, left * 2 + yl, mine):
            term(slot)
        slopes[rows, :] = (slope * scale).astype(BF16)
        share = jnp.sum(slope * value, axis=1, keepdims=True)
        flat = jnp.transpose(jnp.broadcast_to(share, (CHUNK, 128)))[0:8, :]
        line = lax.broadcasted_iota(jnp.int32, (8, CHUNK), 0)
        inner[mine] = jnp.where(line == i, flat, inner[mine])

    each_chunk(second)
    for step in range(1, PARTS):
        there = wrap(mine + step, PARTS)
        remote(
            inner.at[mine],
            inner.at[mine],
            send_sem.at[11],
            inner_sem,
            (z, yh, c, there // 2, lax.rem(there, 2)),
        ).start()

    def grad_of(buffer, l, k):
        return dot(buffer[k], slopes[...], (0, 0)) * FACTOR

    def second_grad(k, carry):
        rows = pl.ds(pl.multiple_of(k * WIDTH, WIDTH), WIDTH)
        grads[0, 1, rows, :] = grad_of(state, 1, k).astype(BF16)
        return carry

    def join(i):
        rows = rows_at(i)
        wait_bytes(ra.at[0, rows], rs_sem.at[0, i])
        slot = across * 2 + yl
        total = terms[slot, rows, :].astype(F32) + ra[0, rows, :].astype(F32)
        terms[slot, rows, :] = total.astype(BF16)
        push(3, terms.at[slot, upper(i)], rb.at[0, i], i, to_right)
        push(4, terms.at[slot, lower(i)], rb.at[1, i], i, to_left)

    def meet(i):
        rows = rows_at(i)
        wait_bytes(ra.at[1, rows], rs_sem.at[1, i])
        wait_bytes(ra.at[2, rows], rs_sem.at[2, i])
        slot = x * 2 + other
        total = (
            terms[slot, rows, :].astype(F32)
            + ra[1, rows, :].astype(F32)
            + ra[2, rows, :].astype(F32)
        )
        terms[slot, rows, :] = total.astype(BF16)
        push(7, terms.at[slot, rows], rc.at[2, rows], i, to_other)

    def pass_on(i):
        rows = rows_at(i)
        wait_bytes(rb.at[0, i], rs_sem.at[3, i])
        slot = right * 2 + yl
        total = terms[slot, upper(i), :].astype(F32) + rb[0, i].astype(F32)
        terms[slot, upper(i), :] = total.astype(BF16)
        push(5, terms.at[slot, rows], rc.at[0, rows], i, to_right)
        wait_bytes(rb.at[1, i], rs_sem.at[4, i])
        slot = left * 2 + yl
        total = terms[slot, lower(i), :].astype(F32) + rb[1, i].astype(F32)
        terms[slot, lower(i), :] = total.astype(BF16)
        push(6, terms.at[slot, rows], rc.at[1, rows], i, to_left)

    each_chunk(lambda i: (join(i), meet(i)))
    each_chunk(pass_on)
    lax.fori_loop(0, PARTS, second_grad, 0)
    wait_bytes(inner.at[pl.ds(0, PARTS - 1)], inner_sem)
    acc[...] = jnp.zeros_like(acc)

    def ready(i):
        rows = rows_at(i)
        line = lax.broadcasted_iota(jnp.int32, (8, CHUNK), 0)
        total = inner[0]
        for k in range(1, PARTS):
            total = total + inner[k]
        flat = jnp.sum(jnp.where(line == i, total, 0.0), axis=0, keepdims=True)
        share = jnp.transpose(jnp.broadcast_to(flat, (128, CHUNK)))[:, 0:1]
        scale = scale1[rows, 0:1]
        raw[0, rows, :] = cot[rows, :].astype(F32) - state[mine, rows, :].astype(F32) * (
            scale * scale * share / D
        )
        raw[1, rows, :] = silu_slope(pre0[rows, :]) * scale0[rows, 0:1]

    each_chunk(ready)

    def finish(i):
        rows = rows_at(i)
        wait_bytes(rc.at[0, rows], rs_sem.at[5, i])
        wait_bytes(rc.at[1, rows], rs_sem.at[6, i])
        wait_bytes(rc.at[2, rows], rs_sem.at[7, i])
        normed_grad = (
            terms[mine, rows, :].astype(F32)
            + rc[0, rows, :].astype(F32)
            + rc[1, rows, :].astype(F32)
            + rc[2, rows, :].astype(F32)
        )
        state_grad = raw[0, rows, :] + scale1[rows, 0:1] * normed_grad
        narrow_slope = (state_grad * raw[1, rows, :]).astype(BF16)
        for k in range(PARTS):
            acc[k] += dot(tok[k, rows, :], narrow_slope, (0, 0))

    each_chunk(finish)

    def first_grad(k, carry):
        rows = pl.ds(pl.multiple_of(k * WIDTH, WIDTH), WIDTH)
        grads[0, 0, rows, :] = (acc[k] * FACTOR).astype(BF16)
        return carry

    lax.fori_loop(0, PARTS, first_grad, 0)

    for p in range(4):
        wait_bytes(send.at[p, pl.ds(0, GROUPS - 1)], send_sem.at[p])
        wait_bytes(relay.at[p], send_sem.at[4 + p])
    wait_bytes(tok.at[pl.ds(0, PARTS - 1)], send_sem.at[8])
    wait_bytes(state.at[pl.ds(0, PARTS - 1)], send_sem.at[9])
    wait_bytes(terms.at[pl.ds(0, PARTS - 1)], send_sem.at[10])
    wait_bytes(inner.at[pl.ds(0, PARTS - 1)], send_sem.at[11])


def store(anchor, momentum, grads, out_anchor, out_momentum, out_grads, sem):
    copies = [
        pltpu.make_async_copy(anchor, out_anchor, sem.at[0]),
        pltpu.make_async_copy(momentum, out_momentum, sem.at[1]),
        pltpu.make_async_copy(grads, out_grads, sem.at[2]),
    ]
    for copy in copies:
        copy.start()
    for copy in copies:
        copy.wait()


def shards(anchor, momentum, deltas, old_path, new_path, tokens, cotangent):
    anywhere = pl.BlockSpec(memory_space=pltpu.HBM)
    dma = pltpu.SemaphoreType.DMA
    held = pl.pallas_call(
        kernel,
        out_shape=(
            pltpu.VMEM(anchor.shape, F32),
            pltpu.VMEM(momentum.shape, F32),
            pltpu.VMEM((1, LEVELS, D, WIDTH), BF16),
        ),
        in_specs=[anywhere] * 7,
        out_specs=(pl.BlockSpec(memory_space=pltpu.VMEM),) * 3,
        scratch_shapes=[
            pltpu.SMEM((LEVELS, GROUPS), jnp.int32),
            pltpu.SMEM((LEVELS, GROUPS), jnp.int32),
            pltpu.VMEM((LEVELS, D, WIDTH), F32),
            pltpu.VMEM((4, GROUPS, BLOCK, WIDTH), BF16),
            pltpu.VMEM((4, GROUPS, BLOCK, WIDTH), BF16),
            pltpu.VMEM((4, RELAYS, BLOCK, WIDTH), BF16),
            pltpu.VMEM((LEVELS * MODS, BLOCK, WIDTH), BF16),
            pltpu.VMEM((LEVELS, MODS * TILE, GROUPS * TILE), BF16),
            pltpu.VMEM((LEVELS, MODS * TILE, 128), F32),
            pltpu.VMEM((PARTS, ROWS, WIDTH), BF16),
            pltpu.VMEM((ROWS, WIDTH), BF16),
            pltpu.VMEM((PARTS, ROWS, WIDTH), BF16),
            pltpu.VMEM((ROWS, WIDTH), F32),
            pltpu.VMEM((ROWS, 128), F32),
            pltpu.VMEM((ROWS, 128), F32),
            pltpu.VMEM((ROWS, WIDTH), BF16),
            pltpu.VMEM((PARTS, ROWS, WIDTH), BF16),
            pltpu.VMEM((3, ROWS, WIDTH), BF16),
            pltpu.VMEM((2, CHUNKS, HALF, WIDTH), BF16),
            pltpu.VMEM((3, ROWS, WIDTH), BF16),
            pltpu.VMEM((PARTS, 8, CHUNK), F32),
            pltpu.VMEM((PARTS, WIDTH, WIDTH), F32),
            dma((8,)),
            dma((12,)),
            dma((4, 2, RELAYS)),
            dma((4, 3)),
            dma((9, CHUNKS)),
            dma((9, CHUNKS)),
            dma((8, CHUNKS)),
            dma(()),
        ],
        compiler_params=pltpu.CompilerParams(
            collective_id=0, has_side_effects=True, vmem_limit_bytes=59 * 1024 * 1024
        ),
    )(old_path.T, new_path.T, anchor, momentum, deltas, tokens, cotangent)
    return pl.pallas_call(
        store,
        out_shape=tuple(jax.ShapeDtypeStruct(part.shape, part.dtype) for part in held),
        in_specs=[pl.BlockSpec(memory_space=pltpu.VMEM)] * 3,
        out_specs=(anywhere,) * 3,
        scratch_shapes=[dma((3,))],
        compiler_params=pltpu.CompilerParams(vmem_limit_bytes=16 * 1024 * 1024),
    )(*held)


def solution(mesh):
    split = Mesh(mesh.devices.reshape(SIZES), AXES)
    placed = (
        P(None, GROUP, MP),
        P(None, GROUP, MP),
        P(GROUP, None, None, MP),
        P(),
        P(),
        P(GROUP, None, MP),
        P(GROUP, None, MP),
    )
    return jax.shard_map(
        shards,
        mesh=split,
        in_specs=placed,
        out_specs=(P(None, GROUP, MP), P(None, GROUP, MP), P(GROUP, None, None, MP)),
        check_vma=False,
    )
```

```python
import math

import jax
import jax.numpy as jnp
from jax import lax
from jax.experimental import pallas as pl
from jax.experimental.pallas import tpu as pltpu
from jax.sharding import Mesh
from jax.sharding import PartitionSpec as P

D = 2048
MODS = 8
GROUPS = 32
ROWS = 1024
LEVELS = 2
BLOCK = D // GROUPS
WIDTH = 256
PARTS = D // WIDTH
CHUNKS = 4
CHUNK = ROWS // CHUNKS
HALF = CHUNK // 2
TILE = 16
PIECE = BLOCK // 2
SPLIT = 1
FACTOR = 1.0 / math.sqrt(D)

outer_rate = 0.7
momentum_rate = 0.9
epsilon = 1e-06

AXES = ("z", "yh", "c", "x", "yl")
SIZES = (8, 2, 2, 4, 2)
GROUP = ("z", "yh", "c")
MP = ("x", "yl")
NEAR = (3, -3, 2, -2, 1, -1, 0)
RELAYS = 18
BF16 = jnp.bfloat16
F32 = jnp.float32


def wrap(value, size):
    return lax.rem(value + size, size)


def sigmoid(values):
    return 1.0 / (1.0 + jnp.exp(-values))


def silu_slope(values):
    part = sigmoid(values)
    return part * (1.0 + values * (1.0 - part))


def dot(a, b, dims):
    return lax.dot_general(a, b, ((dims[0:1], dims[1:2]), ((), ())), preferred_element_type=F32)


def kernel(
    old_table,
    new_table,
    anchor_ref,
    momentum_ref,
    deltas_ref,
    tokens_ref,
    cot_ref,
    anchor,
    momentum,
    grads,
    old_ref,
    new_ref,
    raw,
    send,
    recv,
    relay,
    modules,
    selector,
    count,
    tok,
    cot,
    state,
    pre0,
    scale0,
    scale1,
    slopes,
    terms,
    ra,
    rb,
    rc,
    rd,
    inner,
    acc,
    load_sem,
    send_sem,
    relay_sem,
    recv_sem,
    tok_sem,
    state_sem,
    rs_sem,
    inner_sem,
):
    z = lax.axis_index("z")
    yh = lax.axis_index("yh")
    c = lax.axis_index("c")
    x = lax.axis_index("x")
    yl = lax.axis_index("yl")
    y = yh * 2 + yl
    group = z * 4 + yh * 2 + c
    mine = x * 2 + yl

    load = [
        pltpu.make_async_copy(deltas_ref.at[0, 0], raw.at[0], load_sem.at[0]),
        pltpu.make_async_copy(deltas_ref.at[0, 1], raw.at[1], load_sem.at[1]),
        pltpu.make_async_copy(tokens_ref.at[0], tok.at[mine], load_sem.at[2]),
        pltpu.make_async_copy(cot_ref.at[0], cot, load_sem.at[3]),
        pltpu.make_async_copy(anchor_ref, anchor, load_sem.at[4]),
        pltpu.make_async_copy(momentum_ref, momentum, load_sem.at[5]),
        pltpu.make_async_copy(old_table, old_ref, load_sem.at[6]),
        pltpu.make_async_copy(new_table, new_ref, load_sem.at[7]),
    ]
    for copy in load:
        copy.start()

    def remote(src, dst, sender, receiver, device):
        return pltpu.make_async_remote_copy(
            src_ref=src,
            dst_ref=dst,
            send_sem=sender,
            recv_sem=receiver,
            device_id=device,
            device_id_type=pl.DeviceIdType.MESH,
        )

    def wait_bytes(ref, sem):
        pltpu.make_async_copy(ref, ref, sem).wait()

    def place(dz, dy, core):
        there = wrap(y + dy, 4)
        return (wrap(z + dz, 8), there // 2, core, x, lax.rem(there, 2))

    partners = [place(0, 0, 1 - c)]
    for dz in NEAR:
        if dz != 0:
            partners += [place(dz, 0, 0), place(dz, 0, 1)]
        for dy in (1, -1):
            partners.append(place(dz, dy, c))
            if dz in (0, 2, -2):
                partners.append(place(dz, dy, 1 - c))
    for dx in (1, 2, 3):
        for part in (yl, 1 - yl):
            partners.append((z, yh, c, wrap(x + dx, 4), part))
    barrier = pltpu.get_barrier_semaphore()
    for partner in partners:
        pl.semaphore_signal(
            barrier, inc=1, device_id=partner, device_id_type=pl.DeviceIdType.MESH
        )

    def piece(h):
        return pl.ds(0, BLOCK) if h is None else pl.ds(h * PIECE, PIECE)

    def send_block(p, h, dz, cross, core, dst, receiver, device):
        target = wrap(z + dz, 8) * 4 + lax.rem(yh + cross, 2) * 2 + core
        remote(send.at[p, target, piece(h)], dst, send_sem.at[p], receiver, device).start()

    def send_relayed(p, h=None):
        def go(dz, cross, core, slot, device):
            dst, receiver = relay.at[p, slot, piece(h)], relay_sem.at[p, h or 0, slot]
            send_block(p, h, dz, cross, core, dst, receiver, device)

        for i, sign in enumerate((1, -1)):
            go(4, 1, i, 14 + i, place(2 * sign, sign, c))
            go(4, 0, i, 16 + i, place(2 * sign, 0, c))
        for j, dz in enumerate(NEAR):
            for i, sign in enumerate((1, -1)):
                go(dz, 1, i, i * 7 + j, place(dz, sign, c))

    def send_direct(p, h=None):
        for dz in NEAR:
            for core in (1 - c,) if dz == 0 else (0, 1):
                dst, receiver = recv.at[p, group, piece(h)], recv_sem.at[p, 1 + (h or 0)]
                send_block(p, h, dz, 0, core, dst, receiver, place(dz, 0, core))

    def forward_blocks(p, h=None):
        def go(slot, dz, dy, device):
            source = wrap(z - dz, 8) * 4 + (wrap(y - dy, 4) // 2) * 2 + c
            held = relay.at[p, slot, piece(h)]
            wait_bytes(held, relay_sem.at[p, h or 0, slot])
            dst = recv.at[p, source, piece(h)]
            remote(held, dst, send_sem.at[4 + p], recv_sem.at[p, 0], device).start()

        for i, sign in enumerate((1, -1)):
            go(14 + i, 2 * sign, sign, place(2 * sign, sign, i))
            go(16 + i, 2 * sign, 0, place(2 * sign, 0, i))
        for j, dz in enumerate(NEAR):
            for i, sign in enumerate((1, -1)):
                go(i * 7 + j, dz, sign, place(0, sign, i))

    def arrive_relayed(p):
        wait_bytes(recv.at[p, pl.ds(0, RELAYS)], recv_sem.at[p, 0])

    def arrive_direct(p, h=None):
        near = pl.ds(0, GROUPS - 1 - RELAYS)
        wait_bytes(recv.at[p, near, piece(h)], recv_sem.at[p, 1 + (h or 0)])

    def prepare(l):
        tall = (MODS * TILE, GROUPS * TILE)
        line = lax.broadcasted_iota(jnp.int32, tall, 0)
        lane = lax.broadcasted_iota(jnp.int32, tall, 1)
        owner = lax.broadcasted_iota(jnp.int32, (8, GROUPS * TILE), 1) // TILE
        named = jnp.zeros((8, GROUPS * TILE), jnp.int32)
        for g in range(GROUPS):
            named = jnp.where(owner == g, old_ref[l, g], named)
        wanted = jnp.broadcast_to(named[0:1, :] * TILE, tall) + lane % TILE
        chosen = jnp.where(line == wanted, 1.0, 0.0)
        selector[l] = chosen.astype(BF16)
        count[l] = jnp.broadcast_to(jnp.sum(chosen, axis=1, keepdims=True), (MODS * TILE, 128))

    def update(l, h=None):
        for r in range(BLOCK // TILE) if h is None else range(2 * h, 2 * h + 2):
            rows = pl.ds(r * TILE, TILE)
            values = recv[l, :, rows, :].reshape(GROUPS * TILE, WIDTH)
            sums = dot(selector[l], values, (1, 0)) / count[l][:, 0:1]
            for m in range(MODS):
                k = l * MODS + m
                outer_grad = sums[m * TILE : (m + 1) * TILE]
                fresh = momentum_rate * momentum[k, rows, :] + outer_grad
                moved = anchor[k, rows, :] - outer_rate * (outer_grad + momentum_rate * fresh)
                momentum[k, rows, :] = fresh
                anchor[k, rows, :] = moved
                modules[k, rows, :] = moved.astype(BF16)

        def stage(g, carry):
            send[2 + l, g, piece(h), :] = modules[l * MODS + new_ref[l, g], piece(h), :]
            return carry

        lax.fori_loop(0, GROUPS, stage, 0, unroll=4)
        recv[2 + l, group, piece(h), :] = modules[l * MODS + new_ref[l, group], piece(h), :]

    right, left = wrap(x + 1, 4), wrap(x - 1, 4)
    across = wrap(x + 2, 4)
    other = 1 - yl
    to_right = (z, yh, c, right, yl)
    to_left = (z, yh, c, left, yl)
    to_other = (z, yh, c, x, other)

    def rows_at(i):
        return pl.ds(pl.multiple_of(i * CHUNK, CHUNK), CHUNK)

    def upper(i):
        return pl.ds(pl.multiple_of(i * CHUNK, HALF), HALF)

    def lower(i):
        return pl.ds(pl.multiple_of(i * CHUNK + HALF, HALF), HALF)

    class Gather:
        def __init__(self, buffer, sems, sender):
            self.buffer, self.sems, self.sender = buffer, sems, sender

        def push(self, kind, slot, rows, i, device):
            ref = self.buffer.at[slot, rows]
            remote(ref, ref, self.sender, self.sems.at[kind, i], device).start()

        def wait(self, kind, slot, rows, i):
            wait_bytes(self.buffer.at[slot, rows], self.sems.at[kind, i])

        def own(self, i):
            self.push(2, mine, rows_at(i), i, to_other)
            self.push(0, mine, rows_at(i), i, to_right)
            self.push(1, mine, rows_at(i), i, to_left)

        def halves(self, i):
            self.wait(0, left * 2 + yl, rows_at(i), i)
            self.push(3, left * 2 + yl, upper(i), i, to_right)
            self.wait(1, right * 2 + yl, rows_at(i), i)
            self.push(4, right * 2 + yl, lower(i), i, to_left)

        def pair(self, i):
            self.wait(2, x * 2 + other, rows_at(i), i)
            self.push(5, x * 2 + other, rows_at(i), i, to_right)
            self.push(6, x * 2 + other, rows_at(i), i, to_left)

        def far(self, i):
            self.wait(3, across * 2 + yl, upper(i), i)
            self.wait(4, across * 2 + yl, lower(i), i)
            self.push(7, across * 2 + yl, rows_at(i), i, to_other)

        def far_halves(self, i):
            self.wait(5, left * 2 + other, rows_at(i), i)
            self.push(7, left * 2 + other, upper(i), i, to_right)
            self.wait(6, right * 2 + other, rows_at(i), i)
            self.push(8, right * 2 + other, lower(i), i, to_left)

        def last_halves(self, i):
            self.wait(3, across * 2 + yl, upper(i), i)
            self.wait(4, across * 2 + yl, lower(i), i)
            self.wait(7, across * 2 + other, upper(i), i)
            self.wait(8, across * 2 + other, lower(i), i)

        def last(self, i):
            self.wait(5, left * 2 + other, rows_at(i), i)
            self.wait(6, right * 2 + other, rows_at(i), i)
            self.wait(7, across * 2 + other, rows_at(i), i)

    def each_chunk(body, start=0):
        def step(i, carry):
            body(i)
            return carry

        lax.fori_loop(start, CHUNKS, step, 0)

    def row_scale(buffer, target, i):
        rows = rows_at(i)
        total = jnp.zeros((CHUNK, WIDTH), F32)
        for k in range(PARTS):
            value = buffer[k, rows, :].astype(F32)
            total = total + value * value
        mean = jnp.sum(total, axis=1, keepdims=True) / D
        target[rows, :] = jnp.broadcast_to(lax.rsqrt(mean + epsilon), (CHUNK, 128))

    def weight(l, k):
        return recv[2 + l, pl.ds(4 * k, 4)].reshape(WIDTH, WIDTH)

    def product(buffer, l, i):
        rows = rows_at(i)
        total = dot(buffer[0, rows, :], weight(l, 0), (1, 0))
        for k in range(1, PARTS):
            total = total + dot(buffer[k, rows, :], weight(l, k), (1, 0))
        return total

    def narrow(l):
        def one(g, carry):
            rows = pl.ds(pl.multiple_of(g * BLOCK, BLOCK), BLOCK)
            send[l, g] = raw[l, rows, :].astype(BF16)
            return carry

        lax.fori_loop(0, GROUPS, one, 0)
        recv[l, group] = send[l, group]

    tokens = Gather(tok, tok_sem, send_sem.at[8])
    states = Gather(state, state_sem, send_sem.at[9])

    load[0].wait()
    narrow(0)
    pl.semaphore_wait(barrier, len(partners))
    send_relayed(0)
    send_direct(0)
    load[2].wait()
    each_chunk(tokens.own)
    load[1].wait()
    narrow(1)
    load[6].wait()
    load[7].wait()
    prepare(0)
    prepare(1)
    load[4].wait()
    load[5].wait()
    forward_blocks(0)
    send_relayed(1)
    each_chunk(tokens.halves)
    each_chunk(tokens.pair)
    arrive_relayed(0)
    arrive_direct(0)
    update(0)
    send_relayed(2)
    send_direct(2)
    forward_blocks(1)
    forward_blocks(2)
    send_direct(1, 0)
    send_direct(1, 1)
    each_chunk(tokens.far_halves)
    each_chunk(tokens.last_halves)
    each_chunk(lambda i: row_scale(tok, scale0, i))
    load[3].wait()
    arrive_relayed(2)
    arrive_direct(2)

    def first(i):
        rows = rows_at(i)
        value = product(tok, 0, i) * (scale0[rows, 0:1] * FACTOR)
        pre0[rows, :] = value
        fresh = tok[mine, rows, :].astype(F32) + value * sigmoid(value)
        state[mine, rows, :] = fresh.astype(BF16)
        states.own(i)

    each_chunk(first)
    arrive_relayed(1)
    arrive_direct(1, 0)
    update(1, 0)
    send_relayed(3, 0)
    send_direct(3, 0)
    arrive_direct(1, 1)
    update(1, 1)
    send_relayed(3, 1)
    send_direct(3, 1)
    each_chunk(states.halves)
    forward_blocks(3, 0)
    each_chunk(states.pair)
    states.far(1)
    forward_blocks(3, 1)
    states.far(2)
    states.far(3)
    states.far_halves(0)
    for i in range(CHUNKS):
        if i < SPLIT:
            states.last_halves(i)
        else:
            states.last(i)
    each_chunk(lambda i: row_scale(state, scale1, i))
    arrive_relayed(3)
    arrive_direct(3, 0)
    arrive_direct(3, 1)

    def push(kind, src, dst, i, device):
        remote(src, dst, send_sem.at[10], rs_sem.at[kind, i], device).start()

    inner[mine] = jnp.zeros((8, CHUNK), F32)

    def second(i, detour=False):
        rows = rows_at(i)
        scale = scale1[rows, 0:1]
        value = product(state, 1, i) * (scale * FACTOR)
        slope = cot[rows, :].astype(F32) * silu_slope(value)
        narrow_slope = slope.astype(BF16)

        def term(slot):
            product_of = dot(narrow_slope, weight(1, slot), (1, 1)) * FACTOR
            terms[slot, rows, :] = product_of.astype(BF16)

        outgoing = (
            (across * 2 + other, to_other),
            (right * 2 + other, to_right),
            (left * 2 + other, to_left),
        )
        for kind, (slot, device) in enumerate(outgoing):
            term(slot)
        for kind, (slot, device) in enumerate(outgoing):
            part = upper(i) if detour and kind > 0 else rows
            push(kind, terms.at[slot, part], ra.at[kind, part], i, device)
        for slot in (across * 2 + yl, x * 2 + other, right * 2 + yl, left * 2 + yl, mine):
            term(slot)
        slopes[rows, :] = (slope * scale).astype(BF16)
        share = jnp.sum(slope * value, axis=1, keepdims=True)
        flat = jnp.transpose(jnp.broadcast_to(share, (CHUNK, 128)))[0:8, :]
        line = lax.broadcasted_iota(jnp.int32, (8, CHUNK), 0)
        inner[mine] = jnp.where(line == i, flat, inner[mine])

    second(0, detour=True)
    each_chunk(second, 1)
    for side, slot in enumerate((right * 2 + other, left * 2 + other)):
        push(8, terms.at[slot, lower(0)], rd.at[side], side, to_other)
    for step in range(1, PARTS):
        there = wrap(mine + step, PARTS)
        remote(
            inner.at[mine],
            inner.at[mine],
            send_sem.at[11],
            inner_sem,
            (z, yh, c, there // 2, lax.rem(there, 2)),
        ).start()

    def grad_of(buffer, l, k):
        return dot(buffer[k], slopes[...], (0, 0)) * FACTOR

    def second_grad(k, carry):
        rows = pl.ds(pl.multiple_of(k * WIDTH, WIDTH), WIDTH)
        grads[0, 1, rows, :] = grad_of(state, 1, k).astype(BF16)
        return carry

    def join(i):
        rows = rows_at(i)
        wait_bytes(ra.at[0, rows], rs_sem.at[0, i])
        slot = across * 2 + yl
        total = terms[slot, rows, :].astype(F32) + ra[0, rows, :].astype(F32)
        terms[slot, rows, :] = total.astype(BF16)
        push(3, terms.at[slot, upper(i)], rb.at[0, i], i, to_right)
        push(4, terms.at[slot, lower(i)], rb.at[1, i], i, to_left)

    def meet(i, detour=False):
        rows = upper(i) if detour else rows_at(i)
        wait_bytes(ra.at[1, rows], rs_sem.at[1, i])
        wait_bytes(ra.at[2, rows], rs_sem.at[2, i])
        slot = x * 2 + other
        total = (
            terms[slot, rows, :].astype(F32)
            + ra[1, rows, :].astype(F32)
            + ra[2, rows, :].astype(F32)
        )
        terms[slot, rows, :] = total.astype(BF16)
        push(7, terms.at[slot, rows_at(i)], rc.at[2, rows_at(i)], i, to_other)

    def pass_on(i, detour=False):
        rows = rows_at(i)
        wait_bytes(rb.at[0, i], rs_sem.at[3, i])
        slot = right * 2 + yl
        total = terms[slot, upper(i), :].astype(F32) + rb[0, i].astype(F32)
        terms[slot, upper(i), :] = total.astype(BF16)
        if detour:
            wait_bytes(rd.at[0], rs_sem.at[8, 0])
            total = terms[slot, lower(i), :].astype(F32) + rd[0].astype(F32)
            terms[slot, lower(i), :] = total.astype(BF16)
        push(5, terms.at[slot, rows], rc.at[0, rows], i, to_right)
        wait_bytes(rb.at[1, i], rs_sem.at[4, i])
        slot = left * 2 + yl
        total = terms[slot, lower(i), :].astype(F32) + rb[1, i].astype(F32)
        if detour:
            wait_bytes(rd.at[1], rs_sem.at[8, 1])
            total = total + rd[1].astype(F32)
        terms[slot, lower(i), :] = total.astype(BF16)
        push(6, terms.at[slot, rows], rc.at[1, rows], i, to_left)

    join(0)
    meet(0, detour=True)
    each_chunk(lambda i: (join(i), meet(i)), 1)
    pass_on(0, detour=True)
    each_chunk(pass_on, 1)
    lax.fori_loop(0, PARTS, second_grad, 0)
    wait_bytes(inner.at[pl.ds(0, PARTS - 1)], inner_sem)
    acc[...] = jnp.zeros_like(acc)

    def ready(i):
        rows = rows_at(i)
        line = lax.broadcasted_iota(jnp.int32, (8, CHUNK), 0)
        total = inner[0]
        for k in range(1, PARTS):
            total = total + inner[k]
        flat = jnp.sum(jnp.where(line == i, total, 0.0), axis=0, keepdims=True)
        share = jnp.transpose(jnp.broadcast_to(flat, (128, CHUNK)))[:, 0:1]
        scale = scale1[rows, 0:1]
        raw[0, rows, :] = cot[rows, :].astype(F32) - state[mine, rows, :].astype(F32) * (
            scale * scale * share / D
        )
        raw[1, rows, :] = silu_slope(pre0[rows, :]) * scale0[rows, 0:1]

    each_chunk(ready)

    def finish(i):
        rows = rows_at(i)
        wait_bytes(rc.at[0, rows], rs_sem.at[5, i])
        wait_bytes(rc.at[1, rows], rs_sem.at[6, i])
        wait_bytes(rc.at[2, rows], rs_sem.at[7, i])
        normed_grad = (
            terms[mine, rows, :].astype(F32)
            + rc[0, rows, :].astype(F32)
            + rc[1, rows, :].astype(F32)
            + rc[2, rows, :].astype(F32)
        )
        state_grad = raw[0, rows, :] + scale1[rows, 0:1] * normed_grad
        narrow_slope = (state_grad * raw[1, rows, :]).astype(BF16)
        for k in range(PARTS):
            acc[k] += dot(tok[k, rows, :], narrow_slope, (0, 0))

    each_chunk(finish)

    def first_grad(k, carry):
        rows = pl.ds(pl.multiple_of(k * WIDTH, WIDTH), WIDTH)
        grads[0, 0, rows, :] = (acc[k] * FACTOR).astype(BF16)
        return carry

    lax.fori_loop(0, PARTS, first_grad, 0)

    for p in range(4):
        wait_bytes(send.at[p, pl.ds(0, GROUPS - 1)], send_sem.at[p])
        wait_bytes(relay.at[p], send_sem.at[4 + p])
    wait_bytes(tok.at[pl.ds(0, PARTS - 1)], send_sem.at[8])
    wait_bytes(state.at[pl.ds(0, PARTS - 1)], send_sem.at[9])
    wait_bytes(terms.at[pl.ds(0, PARTS - 1)], send_sem.at[10])
    wait_bytes(inner.at[pl.ds(0, PARTS - 1)], send_sem.at[11])


def store(anchor, momentum, grads, out_anchor, out_momentum, out_grads, sem):
    copies = [
        pltpu.make_async_copy(anchor, out_anchor, sem.at[0]),
        pltpu.make_async_copy(momentum, out_momentum, sem.at[1]),
        pltpu.make_async_copy(grads, out_grads, sem.at[2]),
    ]
    for copy in copies:
        copy.start()
    for copy in copies:
        copy.wait()


def shards(anchor, momentum, deltas, old_path, new_path, tokens, cotangent):
    anywhere = pl.BlockSpec(memory_space=pltpu.HBM)
    dma = pltpu.SemaphoreType.DMA
    held = pl.pallas_call(
        kernel,
        out_shape=(
            pltpu.VMEM(anchor.shape, F32),
            pltpu.VMEM(momentum.shape, F32),
            pltpu.VMEM((1, LEVELS, D, WIDTH), BF16),
        ),
        in_specs=[anywhere] * 7,
        out_specs=(pl.BlockSpec(memory_space=pltpu.VMEM),) * 3,
        scratch_shapes=[
            pltpu.SMEM((LEVELS, GROUPS), jnp.int32),
            pltpu.SMEM((LEVELS, GROUPS), jnp.int32),
            pltpu.VMEM((LEVELS, D, WIDTH), F32),
            pltpu.VMEM((4, GROUPS, BLOCK, WIDTH), BF16),
            pltpu.VMEM((4, GROUPS, BLOCK, WIDTH), BF16),
            pltpu.VMEM((4, RELAYS, BLOCK, WIDTH), BF16),
            pltpu.VMEM((LEVELS * MODS, BLOCK, WIDTH), BF16),
            pltpu.VMEM((LEVELS, MODS * TILE, GROUPS * TILE), BF16),
            pltpu.VMEM((LEVELS, MODS * TILE, 128), F32),
            pltpu.VMEM((PARTS, ROWS, WIDTH), BF16),
            pltpu.VMEM((ROWS, WIDTH), BF16),
            pltpu.VMEM((PARTS, ROWS, WIDTH), BF16),
            pltpu.VMEM((ROWS, WIDTH), F32),
            pltpu.VMEM((ROWS, 128), F32),
            pltpu.VMEM((ROWS, 128), F32),
            pltpu.VMEM((ROWS, WIDTH), BF16),
            pltpu.VMEM((PARTS, ROWS, WIDTH), BF16),
            pltpu.VMEM((3, ROWS, WIDTH), BF16),
            pltpu.VMEM((2, CHUNKS, HALF, WIDTH), BF16),
            pltpu.VMEM((3, ROWS, WIDTH), BF16),
            pltpu.VMEM((2, HALF, WIDTH), BF16),
            pltpu.VMEM((PARTS, 8, CHUNK), F32),
            pltpu.VMEM((PARTS, WIDTH, WIDTH), F32),
            dma((8,)),
            dma((12,)),
            dma((4, 2, RELAYS)),
            dma((4, 3)),
            dma((9, CHUNKS)),
            dma((9, CHUNKS)),
            dma((9, CHUNKS)),
            dma(()),
        ],
        compiler_params=pltpu.CompilerParams(
            collective_id=0, has_side_effects=True, vmem_limit_bytes=59 * 1024 * 1024
        ),
    )(old_path.T, new_path.T, anchor, momentum, deltas, tokens, cotangent)
    return pl.pallas_call(
        store,
        out_shape=tuple(jax.ShapeDtypeStruct(part.shape, part.dtype) for part in held),
        in_specs=[pl.BlockSpec(memory_space=pltpu.VMEM)] * 3,
        out_specs=(anywhere,) * 3,
        scratch_shapes=[dma((3,))],
        compiler_params=pltpu.CompilerParams(vmem_limit_bytes=16 * 1024 * 1024),
    )(*held)


def solution(mesh):
    split = Mesh(mesh.devices.reshape(SIZES), AXES)
    placed = (
        P(None, GROUP, MP),
        P(None, GROUP, MP),
        P(GROUP, None, None, MP),
        P(),
        P(),
        P(GROUP, None, MP),
        P(GROUP, None, MP),
    )
    return jax.shard_map(
        shards,
        mesh=split,
        in_specs=placed,
        out_specs=(P(None, GROUP, MP), P(None, GROUP, MP), P(GROUP, None, None, MP)),
        check_vma=False,
    )
```
